32 devices in a mesh: batch: 1 (over z), ctx: 4 (over y), seq: 8 (over x, core).
Axes of the slice: x: 4, y: 4, z: 1, core: 2. Of those that a mesh axis runs over, the one named last changes fastest.
The devices are a block of a 4x4x8 slice.
Arguments:
- hidden: bfloat16 [16, 5120], P('batch')
- lengths: int32 [16], P('batch')
- latent_cache: bfloat16 [16, 8192, 512], P('batch', ('ctx', 'seq'))
- rope_keys: bfloat16 [16, 8192, 64], P('batch', ('ctx', 'seq'))
- w_uq: bfloat16 [5120, 128, 128], P(None, 'seq')
- w_qr: bfloat16 [5120, 128, 64], P(None, 'seq')
- w_uk: bfloat16 [128, 128, 512], P('seq')
- w_uv: bfloat16 [128, 512, 128], P('seq')
- w_out: bfloat16 [128, 128, 5120], P('seq')
Outputs:
- output: bfloat16 [16, 5120], P('batch')
All inputs are finite; a program needn't handle non-finite values.
Results may differ from the reference program's by a relative error of at most 0.00569913.
Values are sent between devices in bfloat16 or wider.
A program may use at most 768 MiB of HBM per device.

```python
import jax
import jax.numpy as jnp
from jax import lax

NUM_ROWS = 16
SEQ_LEN = 8192
D_MODEL = 5120
NUM_HEADS = 128
LATENT = 512
ROPE_DIM = 64
NOPE_DIM = 128
VALUE_DIM = 128
NUM_WAVES = 3

SCORE_SCALE = (NOPE_DIM + ROPE_DIM) ** -0.5
SHORT_LEN = SEQ_LEN // 8
LONG_LEN = SEQ_LEN - SEQ_LEN // 8


def wave_basis():
    spots = (jnp.arange(SEQ_LEN, dtype=jnp.float32) + 0.5) / SEQ_LEN
    waves = jnp.arange(1, NUM_WAVES + 1, dtype=jnp.float32)
    return jnp.cos(jnp.pi * spots[:, None] * waves[None, :])


def draw_rows(row_keys, width, amplitude, profile):
    def one_row(row_key):
        coef_key, noise_key = jax.random.split(row_key)
        coeffs = amplitude * jax.random.normal(coef_key, (NUM_WAVES, width), jnp.float32)
        noise = jax.random.normal(noise_key, (SEQ_LEN, width), jnp.float32)
        return (0.6 * noise + jnp.dot(profile, coeffs)).astype(jnp.bfloat16)
    return lax.map(one_row, row_keys)


def draw_lengths(len_key):
    coin_key, long_key, short_key = jax.random.split(len_key, 3)
    coins = jax.random.randint(coin_key, (NUM_ROWS,), 0, 2)
    long_lens = jax.random.randint(long_key, (NUM_ROWS,), LONG_LEN, SEQ_LEN + 1)
    short_lens = jax.random.randint(short_key, (NUM_ROWS,), SHORT_LEN, SEQ_LEN + 1)
    lengths = jnp.where(coins == 1, long_lens, short_lens)
    return lengths.at[0].set(SEQ_LEN).at[1].set(SHORT_LEN).astype(jnp.int32)


def setup_inputs(seed: int = 0, part: int = 0) -> dict:
    base_key = jax.random.key(seed)
    part_key = jax.random.fold_in(base_key, part)
    weight_keys = jax.random.split(base_key, 5)
    data_keys = jax.random.split(part_key, 4)
    profile = wave_basis()
    q_scale = 0.6 * D_MODEL ** -0.5
    hidden = jax.random.normal(data_keys[0], (NUM_ROWS, D_MODEL), jnp.float32)
    w_uq = q_scale * jax.random.normal(weight_keys[0], (D_MODEL, NUM_HEADS, NOPE_DIM), jnp.float32)
    w_qr = q_scale * jax.random.normal(weight_keys[1], (D_MODEL, NUM_HEADS, ROPE_DIM), jnp.float32)
    w_uk = NOPE_DIM ** -0.5 * jax.random.normal(weight_keys[2], (NUM_HEADS, NOPE_DIM, LATENT), jnp.float32)
    w_uv = LATENT ** -0.5 * jax.random.normal(weight_keys[3], (NUM_HEADS, LATENT, VALUE_DIM), jnp.float32)
    w_out = (NUM_HEADS * VALUE_DIM) ** -0.5 * jax.random.normal(weight_keys[4], (NUM_HEADS, VALUE_DIM, D_MODEL), jnp.float32)
    return {
        'hidden': hidden.astype(jnp.bfloat16),
        'lengths': draw_lengths(data_keys[1]),
        'latent_cache': draw_rows(jax.random.split(data_keys[2], NUM_ROWS), LATENT, 1.0, profile),
        'rope_keys': draw_rows(jax.random.split(data_keys[3], NUM_ROWS), ROPE_DIM, 2.0, profile),
        'w_uq': w_uq.astype(jnp.bfloat16),
        'w_qr': w_qr.astype(jnp.bfloat16),
        'w_uk': w_uk.astype(jnp.bfloat16),
        'w_uv': w_uv.astype(jnp.bfloat16),
        'w_out': w_out.astype(jnp.bfloat16),
    }


def reference(hidden, lengths, latent_cache, rope_keys, w_uq, w_qr, w_uk, w_uv, w_out):
    q_nope = jnp.dot(hidden, w_uq.reshape(D_MODEL, NUM_HEADS * NOPE_DIM), preferred_element_type=jnp.float32)
    q_nope = q_nope.astype(jnp.bfloat16).reshape(NUM_ROWS, NUM_HEADS, NOPE_DIM)
    q_rope = jnp.dot(hidden, w_qr.reshape(D_MODEL, NUM_HEADS * ROPE_DIM), preferred_element_type=jnp.float32)
    q_rope = q_rope.astype(jnp.bfloat16).reshape(NUM_ROWS, NUM_HEADS, ROPE_DIM)
    q_lat = jnp.einsum('bhk,hkc->bhc', q_nope.astype(jnp.float32), w_uk.astype(jnp.float32)).astype(jnp.bfloat16)
    positions = jnp.arange(SEQ_LEN)

    def one_row(row_data):
        lat_row, rope_row, cache_row, keys_row, length = row_data
        scores = jnp.dot(lat_row, cache_row.T, preferred_element_type=jnp.float32)
        scores = (scores + jnp.dot(rope_row, keys_row.T, preferred_element_type=jnp.float32)) * SCORE_SCALE
        valid = positions[None, :] < length
        scores = jnp.where(valid, scores, -jnp.inf)
        row_max = jnp.max(scores, axis=1, keepdims=True)
        weights = jnp.exp(scores - row_max)
        weight_sum = jnp.sum(weights, axis=1, keepdims=True)
        weighted = jnp.dot(weights.astype(jnp.bfloat16), cache_row, preferred_element_type=jnp.float32)
        return (weighted / weight_sum).astype(jnp.bfloat16)

    lat_out = lax.map(one_row, (q_lat, q_rope, latent_cache, rope_keys, lengths))
    head_vals = jnp.einsum('bhc,hcv->bhv', lat_out.astype(jnp.float32), w_uv.astype(jnp.float32)).astype(jnp.bfloat16)
    mixed = jnp.einsum('bhv,hvd->bd', head_vals.astype(jnp.float32), w_out.astype(jnp.float32))
    return (hidden.astype(jnp.float32) + mixed).astype(jnp.bfloat16)
```

```python
import jax
import jax.numpy as jnp
from jax import lax
from jax.experimental import pallas as pl
from jax.experimental.pallas import tpu as pltpu
from jax.sharding import PartitionSpec as P

NEG_FILL = -1.0e30
LANES = 128
MESH = pl.DeviceIdType.MESH


def decode_kernel(ny, ns, lens, hidden, qn, qr, wuk, cache, rope, wuv, wout, out,
                  cacheb, ropeb, qbuf, part, inbox, wukb, wuvb, woutb, qscr, ybuf, yin, obuf,
                  lsem, csend, crecv, gsend, grecv, rsend, rrecv, ysend, yrecv, osend, orecv):
    nx = ns // 2
    y, s = lax.axis_index("ctx"), lax.axis_index("seq")
    x, c = s // 2, s % 2
    rb, hb = y // 2, y % 2
    t_own, latent = cache.shape[1], cache.shape[2]
    rope_dim = rope.shape[1]
    nope = LANES
    scale = (nope + rope_dim) ** -0.5
    n_pos = 2 * t_own
    cols = hidden.shape[1] // ns

    def at_y(d):
        return {"ctx": (y + d + ny) % ny, "seq": s}

    def at_x(d):
        return {"ctx": y, "seq": ((x + d + nx) % nx) * 2 + c}

    span = pl.ds(c * t_own, t_own)
    local = [
        pltpu.make_async_copy(wuk, wukb, lsem.at[0]),
        pltpu.make_async_copy(cache, cacheb.at[:, span], lsem.at[1]),
        pltpu.make_async_copy(rope, ropeb.at[:, :, span], lsem.at[2]),
        pltpu.make_async_copy(wuv, wuvb, lsem.at[3]),
        pltpu.make_async_copy(wout, woutb, lsem.at[4]),
    ]
    for copy in local[:3]:
        copy.start()

    barrier = pltpu.get_barrier_semaphore()
    for dy in range(ny):
        for ds in range(ns):
            if dy or ds:
                pl.semaphore_signal(barrier, inc=1, device_id={"ctx": (y + dy) % ny, "seq": (s + ds) % ns},
                                    device_id_type=MESH)
    pl.semaphore_wait(barrier, ny * ns - 1)

    mate = {"ctx": y, "seq": s + 1 - 2 * c}
    other = pl.ds((1 - c) * t_own, t_own)
    swap = [
        pltpu.make_async_remote_copy(cache, cacheb.at[:, span], csend.at[0], crecv.at[0], device_id=mate, device_id_type=MESH),
        pltpu.make_async_remote_copy(rope, ropeb.at[:, :, span], csend.at[1], crecv.at[1], device_id=mate, device_id_type=MESH),
    ]
    for copy in swap:
        copy.start()

    nh = qn.shape[1]
    half_h, half_b = nh // 2, qn.shape[0] // 2
    local[0].wait()
    qrows = qn[pl.ds(rb * half_b, half_b)].reshape(half_b * nh, nope)
    head_of = lax.broadcasted_iota(jnp.int32, (half_b * nh, nope), 0) % nh
    big = jnp.concatenate([jnp.where(head_of == h, qrows, jnp.zeros_like(qrows)) for h in range(nh)], axis=1)
    q_lat = jnp.dot(big, wukb[...], preferred_element_type=jnp.float32)
    qscr[:, 0:latent] = q_lat
    qscr[:, latent:latent + rope_dim] = qr[pl.ds(rb * half_b, half_b)].reshape(half_b * nh, rope_dim).astype(jnp.float32)
    qscr[:, latent + rope_dim:] = jnp.zeros((half_b * nh, qscr.shape[1] - latent - rope_dim), jnp.float32)
    for j in range(half_b // 2):
        rows = [qscr[pl.ds(pl.multiple_of((2 * j + i) * nh + hb * half_h, 8), half_h), :] for i in range(2)]
        qbuf[rb, j, hb, x] = jnp.concatenate(rows, axis=0).astype(jnp.bfloat16)

    sends = []

    def send(src, dst, ssem, rsem, to):
        copy = pltpu.make_async_remote_copy(src, dst, ssem, rsem, device_id=to, device_id_type=MESH)
        copy.start()
        sends.append(copy)

    def recv(dst, rsem):
        pltpu.make_async_remote_copy(dst, dst, rsem, rsem, device_id=mate, device_id_type=MESH).wait_recv()

    def rbhb(d):
        yy = (y + d + ny) % ny
        return yy // 2, yy % 2

    def xx(d):
        return (x + d + nx) % nx

    def unit_a(d, a):
        return qbuf.at[rb, a, hb, xx(d)]

    def unit_b(d, a):
        r_, h_ = rbhb(d)
        return qbuf.at[r_, 2 + a, h_, x]

    def line_a(d, a):
        r_, h_ = rbhb(d)
        return qbuf.at[r_, a, h_]

    def line_b(d, a):
        return qbuf.at[:, 2 + a, :, xx(d)]

    def gather_start(k, get, to):
        for a in range(2):
            for i, d in ((0, 1), (2, -1)):
                send(get(0, a), get(0, a), gsend.at[k, i + a], grecv.at[k, i + a], to(d))

    def gather_forward(k, get, to):
        recv(get(-1, 0), grecv.at[k, 0])
        send(get(-1, 0), get(-1, 0), gsend.at[k, 4], grecv.at[k, 4], to(1))
        recv(get(1, 1), grecv.at[k, 3])
        send(get(1, 1), get(1, 1), gsend.at[k, 5], grecv.at[k, 5], to(-1))

    def gather_finish(k, get, a):
        if a == 0:
            recv(get(1, 0), grecv.at[k, 2])
            recv(get(-2, 0), grecv.at[k, 4])
        else:
            recv(get(-1, 1), grecv.at[k, 1])
            recv(get(2, 1), grecv.at[k, 5])

    gather_start(0, unit_a, at_x)
    gather_start(1, unit_b, at_y)
    gather_forward(0, unit_a, at_x)
    gather_forward(1, unit_b, at_y)
    for a in range(2):
        gather_finish(0, unit_a, a)
        for i, d in ((0, 1), (2, -1)):
            send(line_a(0, a), line_a(0, a), gsend.at[2, i + a], grecv.at[2, i + a], at_y(d))
        gather_finish(1, unit_b, a)
        for i, d in ((0, 1), (2, -1)):
            send(line_b(0, a), line_b(0, a), gsend.at[3, i + a], grecv.at[3, i + a], at_x(d))
    for copy in local[3:]:
        copy.start()
    for copy in local[1:3]:
        copy.wait()
    recv(cacheb.at[:, other], crecv.at[0])
    recv(ropeb.at[:, :, other], crecv.at[1])
    gather_forward(2, line_a, at_y)
    gather_forward(3, line_b, at_x)
    gather_finish(2, line_a, 0)
    gather_finish(3, line_b, 0)

    base = (y * ns + 2 * x) * t_own
    n_head = qbuf.shape[2] * qbuf.shape[3] * 8
    lane = lax.broadcasted_iota(jnp.int32, (8, LANES), 1)
    n_slab = latent // LANES

    def stats(groups):
        tile = jnp.zeros((8, LANES), jnp.float32)
        for i, (m_, l_) in enumerate(groups):
            tile = jnp.where((lane >= 32 * i) & (lane < 32 * i + 16), m_, tile)
            tile = jnp.where((lane >= 32 * i + 16) & (lane < 32 * i + 32), l_, tile)
        return tile

    def attend(cls, r):
        j = cls + 2 * (r % 2)
        r_ = r // 2
        q2 = qbuf[r_, j].reshape(2 * n_head, qbuf.shape[5])
        res = []
        for i in range(2):
            b = 4 * r + 2 * cls + i
            sc = lax.dot_general(q2[:, 0:latent], cacheb[b], (((1,), (1,)), ((), ())), preferred_element_type=jnp.float32)
            sc = sc + jnp.dot(q2[:, latent:latent + rope_dim], ropeb[b], preferred_element_type=jnp.float32)
            groups = []
            for x_ in range(nx):
                for h_ in range(2):
                    k = (h_ * nx + x_) * 16 + 8 * i
                    groups.append(sc[k:k + 8])
            sc = jnp.concatenate(groups, axis=0) * scale
            pos = base + lax.broadcasted_iota(jnp.int32, (n_head, n_pos), 1)
            valid = pos < lens[b]
            sc = jnp.where(valid, sc, NEG_FILL)
            m = jnp.max(sc, axis=1, keepdims=True)
            w = jnp.where(valid, jnp.exp(sc - m), 0.0)
            l = jnp.sum(w, axis=1, keepdims=True)
            acc = jnp.dot(w.astype(jnp.bfloat16), cacheb[b], preferred_element_type=jnp.float32)
            res.append((m, l, acc))
        for x_ in range(nx):
            ml = []
            for g in range(4):
                m, l, acc = res[g // 2]
                k = 16 * x_ + 8 * (g % 2)
                ml.append((m[k:k + 8], l[k:k + 8]))
                for n in range(n_slab):
                    part[cls, r, x_, 32 * n + 8 * g:32 * n + 8 * g + 8, :] = acc[k:k + 8, LANES * n:LANES * n + LANES]
            part[cls, r, x_, 32 * n_slab:32 * n_slab + 8, :] = stats(ml)

    def merge(own, box):
        st, si = own[32 * n_slab:32 * n_slab + 8, :], box[32 * n_slab:32 * n_slab + 8, :]
        ml = []
        for g in range(4):
            m1, m2 = st[:, 32 * g:32 * g + 1], si[:, 32 * g:32 * g + 1]
            l1, l2 = st[:, 32 * g + 16:32 * g + 17], si[:, 32 * g + 16:32 * g + 17]
            m = jnp.maximum(m1, m2)
            e1, e2 = jnp.exp(m1 - m), jnp.exp(m2 - m)
            ml.append((m, l1 * e1 + l2 * e2))
            f1, f2 = jnp.broadcast_to(e1, (8, LANES)), jnp.broadcast_to(e2, (8, LANES))
            for n in range(n_slab):
                k = 32 * n + 8 * g
                own[k:k + 8, :] = own[k:k + 8, :] * f1 + box[k:k + 8, :] * f2
        own[32 * n_slab:32 * n_slab + 8, :] = stats(ml)

    def rs_send(cls, r, x_, i, to):
        send(part.at[cls, r, x_], inbox.at[cls, i], rsend.at[cls, i], rrecv.at[cls, i], to)

    def rs_merge(cls, r, x_, i):
        recv(inbox.at[cls, i], rrecv.at[cls, i])
        merge(part.at[cls, r, x_], inbox.at[cls, i])

    def yy(d):
        return (y + d + ny) % ny

    def a_first(r):
        sg = 1 - 2 * (r % 2)
        rs_send(0, r, xx(2), r, at_x(sg))
        rs_send(0, r, xx(-sg), 4 + 2 * r + (1 if sg > 0 else 0), at_x(-sg))

    def a_second(r):
        sg = 1 - 2 * (r % 2)
        rs_merge(0, r, xx(sg), r)
        rs_send(0, r, xx(sg), 4 + 2 * r + (0 if sg > 0 else 1), at_x(sg))

    attend(0, 0)
    a_first(0)
    attend(0, 2)
    a_first(2)
    attend(0, 1)
    a_first(1)
    a_second(0)
    attend(0, 3)
    a_first(3)
    a_second(2)
    gather_finish(2, line_a, 1)
    gather_finish(3, line_b, 1)

    attend(1, yy(2))
    for x_ in range(nx):
        rs_send(1, yy(2), x_, x_, at_y(1 - 2 * (x_ % 2)))
    a_second(1)
    a_second(3)
    attend(1, yy(1))
    for x_ in range(nx):
        if x_ % 2 == 0:
            rs_merge(1, yy(1), x_, x_)
        rs_send(1, yy(1), x_, 4 + 2 * x_, at_y(1))
    attend(1, yy(-1))
    for x_ in range(nx):
        if x_ % 2 == 1:
            rs_merge(1, yy(-1), x_, x_)
        rs_send(1, yy(-1), x_, 4 + 2 * x_ + 1, at_y(-1))

    def a_final(r):
        for i in range(2):
            k = 4 + 2 * r + i
            recv(inbox.at[0, k], rrecv.at[0, k])
            merge(part.at[0, r, x], inbox.at[0, k])

    def b_final(x_):
        for i in range(2):
            k = 4 + 2 * x_ + i
            recv(inbox.at[1, k], rrecv.at[1, k])
            merge(part.at[1, y, x_], inbox.at[1, k])

    sy, sx = 1 - 2 * (x % 2), 1 - 2 * (y % 2)
    a_final(yy(2))
    rs_send(0, yy(2), x, 12, at_y(sy))
    attend(1, y)
    a_final(yy(-sy))
    rs_send(0, yy(-sy), x, 13, at_y(-sy))
    b_final(xx(2))
    rs_send(1, y, xx(2), 12, at_x(sx))
    a_final(yy(sy))
    rs_merge(0, yy(sy), x, 12)
    rs_send(0, yy(sy), x, 14, at_y(sy))
    b_final(xx(-sx))
    rs_send(1, y, xx(-sx), 13, at_x(-sx))
    b_final(xx(sx))
    rs_merge(1, y, xx(sx), 12)
    rs_send(1, y, xx(sx), 14, at_x(sx))
    a_final(y)
    b_final(x)
    for i in (13, 14):
        rs_merge(0, y, x, i)
        rs_merge(1, y, x, i)

    rows = []
    for cls in range(2):
        own = part.at[cls, y, x]
        st = own[32 * n_slab:32 * n_slab + 8, :]
        for g in range(4):
            inv = jnp.broadcast_to(st[:, 32 * g + 16:32 * g + 17], (8, LANES))
            rows.append(jnp.concatenate([own[32 * n + 8 * g:32 * n + 8 * g + 8, :] / inv for n in range(n_slab)], axis=1))
    o_l = jnp.concatenate(rows, axis=0).astype(jnp.bfloat16)
    n_own = o_l.shape[0]
    local[3].wait()
    head_o = lax.broadcasted_iota(jnp.int32, (n_own, wuv.shape[2]), 0) % nh
    v = jnp.zeros((n_own, wuv.shape[2]), jnp.float32)
    for h in range(nh):
        v = jnp.where(head_o == h, jnp.dot(o_l, wuvb[h], preferred_element_type=jnp.float32), v)
    v = v.astype(jnp.bfloat16)
    pi = lax.broadcasted_iota(jnp.int32, (16 * nh, n_own), 0)
    pj = lax.broadcasted_iota(jnp.int32, (16 * nh, n_own), 1)
    perm = jnp.where((pj % nh == pi // 16) & (pj // nh == pi % 16), 1.0, 0.0).astype(jnp.bfloat16)
    vp = jnp.dot(perm, v, preferred_element_type=jnp.float32).astype(jnp.bfloat16)
    lhs = jnp.concatenate([vp[16 * h:16 * h + 16] for h in range(nh)], axis=1)
    local[4].wait()
    n_rows = n_own // nh
    for k in range(1, ns + 1):
        s_ = (s + k) % ns
        piece = jnp.dot(lhs, woutb[:, pl.ds(pl.multiple_of(s_ * cols, LANES), cols)], preferred_element_type=jnp.float32)
        if k < ns:
            ybuf[k] = piece[0:n_rows]
            send(ybuf.at[k], yin.at[ns - k], ysend.at[k], yrecv.at[ns - k], {"ctx": y, "seq": s_})
        else:
            total = piece[0:n_rows]
    for k in range(1, ns):
        recv(yin.at[k], yrecv.at[k])
        total = total + yin[k]
    hid = hidden[:, pl.ds(pl.multiple_of(s * cols, LANES), cols)].astype(jnp.float32)
    mine = hid[0:n_rows]
    for y_ in range(1, ny):
        mine = jnp.where(y == y_, hid[n_rows * y_:n_rows * y_ + n_rows], mine)
    obuf[y * ns + s] = (mine + total).astype(jnp.bfloat16)
    me = y * ns + s
    for k in range(1, ny * ns):
        to = (me + k) % (ny * ns)
        send(obuf.at[me], obuf.at[me], osend.at[k], orecv.at[k], {"ctx": to // ns, "seq": to % ns})
    for k in range(1, ny * ns):
        recv(obuf.at[(me + ny * ns - k) % (ny * ns)], orecv.at[k])
    out[...] = obuf[...]
    for copy in sends:
        copy.wait_send()
    for copy in swap:
        copy.wait_send()


def solution(mesh):
    ny, ns = mesh.shape['ctx'], mesh.shape['seq']
    row_spec = P('batch', None)
    cache_spec = P('batch', ('ctx', 'seq'), None)
    proj_spec = P(None, 'seq', None)
    head_spec = P('seq', None, None)

    def local_step(hidden, lengths, latent_cache, rope_keys, w_uq, w_qr, w_uk, w_uv, w_out):
        q_nope = jnp.einsum('bd,dhk->bhk', hidden, w_uq, preferred_element_type=jnp.float32).astype(jnp.bfloat16)
        q_rope = jnp.einsum('bd,dhr->bhr', hidden, w_qr, preferred_element_type=jnp.float32).astype(jnp.bfloat16)
        rope_t = jnp.transpose(rope_keys, (0, 2, 1))
        nb, d_model = hidden.shape
        t_own, latent = latent_cache.shape[1:]
        nh = w_uq.shape[1]
        rope_dim = rope_t.shape[1]
        nx = ns // 2
        cols = d_model // ns
        n_rows = nb // ny
        bf, f32 = jnp.bfloat16, jnp.float32
        unit = (latent // LANES) * 32 + 8
        wide = latent + LANES
        dma = pltpu.SemaphoreType.DMA
        vmem = pl.BlockSpec(memory_space=pltpu.VMEM)
        anyw = pl.BlockSpec(memory_space=pl.ANY)
        import functools
        out = pl.pallas_call(
            functools.partial(decode_kernel, ny, ns),
            out_shape=jax.ShapeDtypeStruct((ny * ns, n_rows, cols), bf),
            in_specs=[pl.BlockSpec(memory_space=pltpu.SMEM), vmem, vmem, vmem, anyw, anyw, anyw, anyw, anyw],
            out_specs=vmem,
            scratch_shapes=[
                pltpu.VMEM((nb, 2 * t_own, latent), bf),
                pltpu.VMEM((nb, rope_dim, 2 * t_own), bf),
                pltpu.VMEM((2, nb // 4, 2, nx, 16, wide), bf),
                pltpu.VMEM((2, ny, nx, unit, LANES), f32),
                pltpu.VMEM((2, 15, unit, LANES), f32),
                pltpu.VMEM((w_uk.shape[0] * w_uk.shape[1], latent), bf),
                pltpu.VMEM(w_uv.shape, bf),
                pltpu.VMEM((w_out.shape[0] * w_out.shape[1], d_model), bf),
                pltpu.VMEM((nb // 2 * nh, wide), f32),
                pltpu.VMEM((ns, n_rows, cols), f32),
                pltpu.VMEM((ns, n_rows, cols), f32),
                pltpu.VMEM((ny * ns, n_rows, cols), bf),
                dma((5,)), dma((2,)), dma((2,)), dma((4, 6)), dma((4, 6)), dma((2, 15)), dma((2, 15)),
                dma((ns,)), dma((ns,)), dma((ny * ns,)), dma((ny * ns,)),
            ],
            compiler_params=pltpu.CompilerParams(collective_id=0, has_side_effects=True, vmem_limit_bytes=60 * 2 ** 20),
        )(lengths, hidden, q_nope, q_rope, w_uk.reshape(-1, latent), latent_cache, rope_t, w_uv, w_out.reshape(-1, d_model))
        out = out.reshape(ny, ns, n_rows, cols)
        return jnp.transpose(out, (0, 2, 1, 3)).reshape(nb, d_model)

    return jax.shard_map(local_step, mesh=mesh,
                         in_specs=(row_spec, P('batch'), cache_spec, cache_spec, proj_spec, proj_spec, head_spec, head_spec, head_spec),
                         out_specs=row_spec, check_vma=False)
```

```python
import jax
import jax.numpy as jnp
from jax import lax
from jax.experimental import pallas as pl
from jax.experimental.pallas import tpu as pltpu
from jax.sharding import PartitionSpec as P

NEG_FILL = -1.0e30
LANES = 128
MESH = pl.DeviceIdType.MESH


def decode_kernel(ny, ns, lens, hidden, wuq, wqr, wuk, cache, rope, wuv, wout, out,
                  cacheb, ropeb, qbuf, part, inbox, wukb, wuvb, woutb, wuqb, wqrb, hrep, ybuf, yin, obuf,
                  lsem, usem, qsem, csend, crecv, gsend, grecv, rsend, rrecv, ysend, yrecv, osend, orecv):
    nx = ns // 2
    y, s = lax.axis_index("ctx"), lax.axis_index("seq")
    x, c = s // 2, s % 2
    rb, hb = y // 2, y % 2
    t_own, latent = cache.shape[1], cache.shape[2]
    rope_dim = rope.shape[1]
    nope = wuq.shape[3]
    d_model = hidden.shape[1]
    nh = wuk.shape[0]
    half_h = wuq.shape[2]
    nb = hidden.shape[0]
    half_b = nb // 2
    scale = (nope + rope_dim) ** -0.5
    n_pos = 2 * t_own
    cols = hidden.shape[1] // ns

    def at_y(d):
        return {"ctx": (y + d + ny) % ny, "seq": s}

    def at_x(d):
        return {"ctx": y, "seq": ((x + d + nx) % nx) * 2 + c}

    step = 256
    n_step = d_model // step
    r_step = 2
    group = 4
    uq = [pltpu.make_async_copy(wuq.at[pl.ds(k * step * group, step * group), hb], wuqb.at[pl.ds(k * step * group, step * group)], usem.at[k])
          for k in range(n_step // group)]
    qr = [pltpu.make_async_copy(wqr.at[pl.ds(hb * half_h + k * r_step, r_step)], wqrb.at[pl.ds(k * r_step, r_step)], qsem.at[k])
          for k in range(half_h // r_step)]
    span = pl.ds(c * t_own, t_own)
    local = [
        pltpu.make_async_copy(wuk.at[pl.ds(hb * half_h, half_h)], wukb, lsem.at[0]),
        pltpu.make_async_copy(cache, cacheb.at[:, span], lsem.at[1]),
        pltpu.make_async_copy(rope, ropeb.at[:, :, span], lsem.at[2]),
        pltpu.make_async_copy(wuv, wuvb, lsem.at[3]),
        pltpu.make_async_copy(wout, woutb, lsem.at[4]),
    ]
    for copy in qr + uq:
        copy.start()

    barrier = pltpu.get_barrier_semaphore()
    for dy in range(ny):
        for ds in range(ns):
            if dy or ds:
                pl.semaphore_signal(barrier, inc=1, device_id={"ctx": (y + dy) % ny, "seq": (s + ds) % ns},
                                    device_id_type=MESH)

    wide_k = step * half_h
    si = lax.broadcasted_iota(jnp.int32, (2 * half_b, nb), 0)
    sj = lax.broadcasted_iota(jnp.int32, (2 * half_b, nb), 1)
    own_rows = jnp.where(sj == rb * half_b + si % half_b, 1.0, 0.0).astype(jnp.bfloat16)
    hid2 = jnp.dot(own_rows, hidden[...], preferred_element_type=jnp.float32).astype(jnp.bfloat16)
    stack = jnp.concatenate([hid2[:, step * k:step * k + step] for k in range(n_step)], axis=0)
    for n in range(half_h):
        ri = lax.broadcasted_iota(jnp.int32, (step, step), 0)
        rj = lax.broadcasted_iota(jnp.int32, (step, step), 1)
        spread = jnp.where(ri == (rj + n * step) // half_h, 1.0, 0.0).astype(jnp.bfloat16)
        hrep[:, n * step:(n + 1) * step] = jnp.dot(stack, spread, preferred_element_type=jnp.float32).astype(jnp.bfloat16)

    pl.semaphore_wait(barrier, ny * ns - 1)

    mate = {"ctx": y, "seq": s + 1 - 2 * c}
    other = pl.ds((1 - c) * t_own, t_own)
    swap = [
        pltpu.make_async_remote_copy(cache, cacheb.at[:, span], csend.at[0], crecv.at[0], device_id=mate, device_id_type=MESH),
        pltpu.make_async_remote_copy(rope, ropeb.at[:, :, span], csend.at[1], crecv.at[1], device_id=mate, device_id_type=MESH),
    ]
    for copy in swap:
        copy.start()

    q_rope = []
    for copy in qr:
        copy.wait()
    for k in range(half_h // r_step):
        w = wqrb[k * r_step:(k + 1) * r_step].reshape(r_step * rope_dim, d_model)
        q_rope.append(lax.dot_general(w, hid2, (((1,), (1,)), ((), ())), preferred_element_type=jnp.float32))
    q_rope = jnp.concatenate(q_rope, axis=0).T
    q_rope = jnp.concatenate([q_rope[0:half_b, rope_dim * h:rope_dim * (h + 1)] for h in range(half_h)], axis=0).astype(jnp.bfloat16)
    lane_h = lax.broadcasted_iota(jnp.int32, (2 * half_b, wide_k), 1) % half_h
    row_h = lax.broadcasted_iota(jnp.int32, (2 * half_b, wide_k), 0) // half_b
    sums = [jnp.zeros((half_h * half_b, nope), jnp.float32) for _ in range(2)]
    for g in range(n_step // group):
        uq[g].wait()
        for k in range(g * group, (g + 1) * group):
            hr = hrep[2 * half_b * k:2 * half_b * (k + 1), :]
            lhs = jnp.concatenate([jnp.where(lane_h == row_h + h, hr, jnp.zeros_like(hr)) for h in range(0, half_h, 2)], axis=0)
            w = wuqb[k * step:(k + 1) * step].reshape(wide_k, nope)
            sums[k % 2] = sums[k % 2] + jnp.dot(lhs, w, preferred_element_type=jnp.float32)
        if g == 2:
            for copy in local[:3]:
                copy.start()
    q_nope = (sums[0] + sums[1]).astype(jnp.bfloat16)

    n_q = half_b * half_h
    qi = lax.broadcasted_iota(jnp.int32, (n_q, n_q), 0)
    qj = lax.broadcasted_iota(jnp.int32, (n_q, n_q), 1)
    pick = jnp.where((qi % half_h == qj // half_b) & (qi // half_h == qj % half_b), 1.0, 0.0).astype(jnp.bfloat16)
    q_nope = jnp.dot(pick, q_nope, preferred_element_type=jnp.float32).astype(jnp.bfloat16)
    q_rope = jnp.dot(pick, q_rope, preferred_element_type=jnp.float32).astype(jnp.bfloat16)
    head_of = lax.broadcasted_iota(jnp.int32, (n_q, nope), 0) % half_h
    big = jnp.concatenate([jnp.where(head_of == h, q_nope, jnp.zeros_like(q_nope)) for h in range(half_h)], axis=1)
    local[0].wait()
    q_lat = jnp.dot(big, wukb[...].reshape(half_h * nope, latent), preferred_element_type=jnp.float32).astype(jnp.bfloat16)
    q_rope = jnp.concatenate([q_rope, jnp.zeros((n_q, LANES - rope_dim), jnp.bfloat16)], axis=1)
    for j in range(half_b // 2):
        qbuf[rb, j, hb, x, :, 0:latent] = q_lat[16 * j:16 * j + 16]
        qbuf[rb, j, hb, x, :, latent:] = q_rope[16 * j:16 * j + 16]

    sends = []

    def send(src, dst, ssem, rsem, to):
        copy = pltpu.make_async_remote_copy(src, dst, ssem, rsem, device_id=to, device_id_type=MESH)
        copy.start()
        sends.append(copy)

    def recv(dst, rsem):
        pltpu.make_async_remote_copy(dst, dst, rsem, rsem, device_id=mate, device_id_type=MESH).wait_recv()

    def rbhb(d):
        yy = (y + d + ny) % ny
        return yy // 2, yy % 2

    def xx(d):
        return (x + d + nx) % nx

    def cell(j, d1, d2):
        d_y, d_x = (d2, d1) if j < 2 else (d1, d2)
        r_, h_ = rbhb(-d_y)
        return qbuf.at[r_, j, h_, xx(-d_x)]

    def hop(j, stage, ref, along_x):
        for d in (2, 1, 3):
            send(ref, ref, gsend.at[j, stage, d], grecv.at[j, stage, d], at_x(d) if along_x else at_y(d))

    for a in range(2):
        for j in (a, a + 2):
            hop(j, 0, cell(j, 0, 0), j < 2)
        for j in (a, a + 2):
            hop(j, 1, cell(j, 0, 0), j >= 2)
    for a in range(2):
        for e in (1, 3, 2):
            for j in (a, a + 2):
                recv(cell(j, e, 0), grecv.at[j, 0, e])
                hop(j, 1 + e, cell(j, e, 0), j >= 2)

    def gather_finish(j):
        for e in range(4):
            for d in (1, 3, 2):
                recv(cell(j, e, d), grecv.at[j, 1 + e, d])

    for copy in local[3:]:
        copy.start()
    for copy in local[1:3]:
        copy.wait()
    recv(cacheb.at[:, other], crecv.at[0])
    recv(ropeb.at[:, :, other], crecv.at[1])
    gather_finish(0)
    gather_finish(2)

    base = (y * ns + 2 * x) * t_own
    n_head = qbuf.shape[2] * qbuf.shape[3] * 8
    lane = lax.broadcasted_iota(jnp.int32, (8, LANES), 1)
    n_slab = latent // LANES

    def stats(groups):
        tile = jnp.zeros((8, LANES), jnp.float32)
        for i, (m_, l_) in enumerate(groups):
            tile = jnp.where((lane >= 32 * i) & (lane < 32 * i + 16), m_, tile)
            tile = jnp.where((lane >= 32 * i + 16) & (lane < 32 * i + 32), l_, tile)
        return tile

    def attend(cls, r):
        j = cls + 2 * (r % 2)
        r_ = r // 2
        q2 = qbuf[r_, j].reshape(2 * n_head, qbuf.shape[5])
        res = []
        for i in range(2):
            b = 4 * r + 2 * cls + i
            sc = lax.dot_general(q2[:, 0:latent], cacheb[b], (((1,), (1,)), ((), ())), preferred_element_type=jnp.float32)
            sc = sc + jnp.dot(q2[:, latent:latent + rope_dim], ropeb[b], preferred_element_type=jnp.float32)
            groups = []
            for x_ in range(nx):
                for h_ in range(2):
                    k = (h_ * nx + x_) * 16 + 8 * i
                    groups.append(sc[k:k + 8])
            sc = jnp.concatenate(groups, axis=0) * scale
            pos = base + lax.broadcasted_iota(jnp.int32, (n_head, n_pos), 1)
            valid = pos < lens[b]
            sc = jnp.where(valid, sc, NEG_FILL)
            m = jnp.max(sc, axis=1, keepdims=True)
            w = jnp.where(valid, jnp.exp(sc - m), 0.0)
            l = jnp.sum(w, axis=1, keepdims=True)
            acc = jnp.dot(w.astype(jnp.bfloat16), cacheb[b], preferred_element_type=jnp.float32)
            res.append((m, l, acc))
        for x_ in range(nx):
            ml = []
            for g in range(4):
                m, l, acc = res[g // 2]
                k = 16 * x_ + 8 * (g % 2)
                ml.append((m[k:k + 8], l[k:k + 8]))
                for n in range(n_slab):
                    part[cls, r, x_, 32 * n + 8 * g:32 * n + 8 * g + 8, :] = acc[k:k + 8, LANES * n:LANES * n + LANES]
            part[cls, r, x_, 32 * n_slab:32 * n_slab + 8, :] = stats(ml)

    def merge(own, box):
        st, si = own[32 * n_slab:32 * n_slab + 8, :], box[32 * n_slab:32 * n_slab + 8, :]
        ml = []
        for g in range(4):
            m1, m2 = st[:, 32 * g:32 * g + 1], si[:, 32 * g:32 * g + 1]
            l1, l2 = st[:, 32 * g + 16:32 * g + 17], si[:, 32 * g + 16:32 * g + 17]
            m = jnp.maximum(m1, m2)
            e1, e2 = jnp.exp(m1 - m), jnp.exp(m2 - m)
            ml.append((m, l1 * e1 + l2 * e2))
            f1, f2 = jnp.broadcast_to(e1, (8, LANES)), jnp.broadcast_to(e2, (8, LANES))
            for n in range(n_slab):
                k = 32 * n + 8 * g
                own[k:k + 8, :] = own[k:k + 8, :] * f1 + box[k:k + 8, :] * f2
        own[32 * n_slab:32 * n_slab + 8, :] = stats(ml)

    def rs_send(cls, r, x_, i, to):
        send(part.at[cls, r, x_], inbox.at[cls, i], rsend.at[cls, i], rrecv.at[cls, i], to)

    def rs_merge(cls, r, x_, i):
        recv(inbox.at[cls, i], rrecv.at[cls, i])
        merge(part.at[cls, r, x_], inbox.at[cls, i])

    def yy(d):
        return (y + d + ny) % ny

    def a_first(r):
        sg = 1 - 2 * (r % 2)
        rs_send(0, r, xx(2), r, at_x(sg))
        rs_send(0, r, xx(-sg), 4 + 2 * r + (1 + sg) // 2, at_x(-sg))

    def a_second(r):
        sg = 1 - 2 * (r % 2)
        rs_merge(0, r, xx(sg), r)
        rs_send(0, r, xx(sg), 4 + 2 * r + (1 - sg) // 2, at_x(sg))

    def b_send(d, odd):
        for x_ in range(odd, nx, 2):
            rs_send(1, yy(d), x_, 4 + 2 * x_ + (1 - d) // 2, at_y(d))

    def b_second(d, odd):
        for x_ in range(odd, nx, 2):
            rs_merge(1, yy(d), x_, x_)
            rs_send(1, yy(d), x_, 4 + 2 * x_ + (1 - d) // 2, at_y(d))

    def a_final(r):
        for i in range(2):
            rs_merge(0, r, x, 4 + 2 * r + i)

    def b_final(x_):
        for i in range(2):
            rs_merge(1, y, x_, 4 + 2 * x_ + i)

    attend(0, yy(2))
    a_first(yy(2))
    attend(0, yy(1))
    a_first(yy(1))
    attend(0, yy(-1))
    a_first(yy(-1))
    a_second(yy(2))
    attend(0, y)
    a_first(y)
    a_second(yy(1))
    gather_finish(1)
    gather_finish(3)
    attend(1, yy(2))
    for x_ in range(nx):
        rs_send(1, yy(2), x_, x_, at_y(1 - 2 * (x_ % 2)))
    a_second(yy(-1))
    attend(1, yy(1))
    b_send(1, 1)
    a_second(y)
    attend(1, yy(-1))
    b_send(-1, 0)
    b_second(1, 0)
    b_second(-1, 1)
    for d in (2, 1, 3):
        a_final(yy(d))
        rs_send(0, yy(d), x, 11 + d, at_y(d))
    attend(1, y)
    for d in (2, 1, 3):
        b_final(xx(d))
        rs_send(1, y, xx(d), 11 + d, at_x(d))
    a_final(y)
    b_final(x)
    for d in (1, 3, 2):
        rs_merge(0, y, x, 11 + d)
        rs_merge(1, y, x, 11 + d)

    rows = []
    for cls in range(2):
        own = part.at[cls, y, x]
        st = own[32 * n_slab:32 * n_slab + 8, :]
        for g in range(4):
            inv = jnp.broadcast_to(st[:, 32 * g + 16:32 * g + 17], (8, LANES))
            rows.append(jnp.concatenate([own[32 * n + 8 * g:32 * n + 8 * g + 8, :] / inv for n in range(n_slab)], axis=1))
    o_l = jnp.concatenate(rows, axis=0).astype(jnp.bfloat16)
    n_own = o_l.shape[0]
    local[3].wait()
    head_o = lax.broadcasted_iota(jnp.int32, (n_own, wuv.shape[2]), 0) % nh
    v = jnp.zeros((n_own, wuv.shape[2]), jnp.float32)
    for h in range(nh):
        v = jnp.where(head_o == h, jnp.dot(o_l, wuvb[h], preferred_element_type=jnp.float32), v)
    v = v.astype(jnp.bfloat16)
    pi = lax.broadcasted_iota(jnp.int32, (16 * nh, n_own), 0)
    pj = lax.broadcasted_iota(jnp.int32, (16 * nh, n_own), 1)
    perm = jnp.where((pj % nh == pi // 16) & (pj // nh == pi % 16), 1.0, 0.0).astype(jnp.bfloat16)
    vp = jnp.dot(perm, v, preferred_element_type=jnp.float32).astype(jnp.bfloat16)
    lhs = jnp.concatenate([vp[16 * h:16 * h + 16] for h in range(nh)], axis=1)
    local[4].wait()
    n_rows = n_own // nh
    others = [(d, f) for d in (2, 1, 3, 0) for f in (0, 1) if (d, f) != (0, 0)]
    for d, f in others + [(0, 0)]:
        s_ = xx(d) * 2 + (1 - c if f else c)
        piece = jnp.dot(lhs, woutb[:, pl.ds(pl.multiple_of(s_ * cols, LANES), cols)], preferred_element_type=jnp.float32)
        if (d, f) != (0, 0):
            k = 2 * d + f
            k_there = 2 * ((nx - d) % nx) + f
            ybuf[k] = piece[0:n_rows]
            send(ybuf.at[k], yin.at[k_there], ysend.at[k], yrecv.at[k_there], {"ctx": y, "seq": s_})
        else:
            total = piece[0:n_rows]
    for d, f in others:
        recv(yin.at[2 * d + f], yrecv.at[2 * d + f])
        total = total + yin[2 * d + f]
    hid = hidden[:, pl.ds(pl.multiple_of(s * cols, LANES), cols)].astype(jnp.float32)
    mine = hid[0:n_rows]
    for y_ in range(1, ny):
        mine = jnp.where(y == y_, hid[n_rows * y_:n_rows * y_ + n_rows], mine)
    obuf[y * ns + s] = (mine + total).astype(jnp.bfloat16)
    me = y * ns + s
    far = [(e, d, f) for e in (2, 1, 3, 0) for d in (2, 1, 3, 0) for f in (0, 1) if (e, d, f) != (0, 0, 0)]
    far.sort(key=lambda t: -(min(t[0], ny - t[0]) + min(t[1], nx - t[1])))
    for e, d, f in far:
        k = (e * nx + d) * 2 + f
        send(obuf.at[me], obuf.at[me], osend.at[k], orecv.at[k], {"ctx": yy(e), "seq": xx(d) * 2 + (1 - c if f else c)})
    for e, d, f in reversed(far):
        recv(obuf.at[yy(-e) * ns + xx(-d) * 2 + (1 - c if f else c)], orecv.at[(e * nx + d) * 2 + f])
    for s_ in range(ns):
        out[:, s_ * cols:(s_ + 1) * cols] = jnp.concatenate(
            [obuf[y_ * ns + s_].astype(jnp.float32) for y_ in range(ny)], axis=0).astype(jnp.bfloat16)
    for copy in sends:
        copy.wait_send()
    for copy in swap:
        copy.wait_send()


def solution(mesh):
    ny, ns = mesh.shape['ctx'], mesh.shape['seq']
    row_spec = P('batch', None)
    cache_spec = P('batch', ('ctx', 'seq'), None)
    proj_spec = P(None, 'seq', None)
    head_spec = P('seq', None, None)

    def local_step(hidden, lengths, latent_cache, rope_keys, w_uq, w_qr, w_uk, w_uv, w_out):
        rope_t = jnp.transpose(rope_keys, (0, 2, 1))
        nb, d_model = hidden.shape
        t_own, latent = latent_cache.shape[1:]
        nh = w_uq.shape[1]
        wqr_t = jnp.transpose(w_qr, (1, 2, 0))
        rope_dim = rope_t.shape[1]
        nx = ns // 2
        cols = d_model // ns
        n_rows = nb // ny
        bf, f32 = jnp.bfloat16, jnp.float32
        unit = (latent // LANES) * 32 + 8
        wide = latent + LANES
        dma = pltpu.SemaphoreType.DMA
        vmem = pl.BlockSpec(memory_space=pltpu.VMEM)
        anyw = pl.BlockSpec(memory_space=pl.ANY)
        import functools
        out = pl.pallas_call(
            functools.partial(decode_kernel, ny, ns),
            out_shape=jax.ShapeDtypeStruct(hidden.shape, bf),
            in_specs=[pl.BlockSpec(memory_space=pltpu.SMEM), vmem, anyw, anyw, anyw, anyw, anyw, anyw, anyw],
            out_specs=vmem,
            scratch_shapes=[
                pltpu.VMEM((nb, 2 * t_own, latent), bf),
                pltpu.VMEM((nb, rope_dim, 2 * t_own), bf),
                pltpu.VMEM((2, nb // 4, 2, nx, 16, wide), bf),
                pltpu.VMEM((2, ny, nx, unit, LANES), f32),
                pltpu.VMEM((2, 15, unit, LANES), f32),
                pltpu.VMEM((nh // 2,) + w_uk.shape[1:], bf),
                pltpu.VMEM(w_uv.shape, bf),
                pltpu.VMEM((w_out.shape[0] * w_out.shape[1], d_model), bf),
                pltpu.VMEM((d_model, nh // 2, w_uq.shape[2]), bf),
                pltpu.VMEM((nh // 2, rope_dim, d_model), bf),
                pltpu.VMEM((d_model // 256 * 16, 256 * nh // 2), bf),
                pltpu.VMEM((ns, n_rows, cols), f32),
                pltpu.VMEM((ns, n_rows, cols), f32),
                pltpu.VMEM((ny * ns, n_rows, cols), bf),
                dma((5,)), dma((d_model // 256,)), dma((nh // 4,)), dma((2,)), dma((2,)), dma((4, 5, 4)), dma((4, 5, 4)), dma((2, 15)), dma((2, 15)),
                dma((ns,)), dma((ns,)), dma((ny * ns,)), dma((ny * ns,)),
            ],
            compiler_params=pltpu.CompilerParams(collective_id=0, has_side_effects=True, vmem_limit_bytes=60 * 2 ** 20),
        )(lengths, hidden, w_uq.reshape(d_model, 2, nh // 2, -1), wqr_t, w_uk, latent_cache, rope_t, w_uv, w_out.reshape(-1, d_model))
        return out

    return jax.shard_map(local_step, mesh=mesh,
                         in_specs=(row_spec, P('batch'), cache_spec, cache_spec, proj_spec, proj_spec, head_spec, head_spec, head_spec),
                         out_specs=row_spec, check_vma=False)
```

```python
import jax
import jax.numpy as jnp
from jax import lax
from jax.experimental import pallas as pl
from jax.experimental.pallas import tpu as pltpu
from jax.sharding import PartitionSpec as P

NEG_FILL = -3.0e38
MAX_FLOOR = -1.5e38
LANES = 128
MESH = pl.DeviceIdType.MESH


def decode_kernel(ny, ns, lens, hidden, wuq, wqr, wuk, cache, rope, wuv, wout, out,
                  cacheb, ropeb, qbuf, part, inbox, wukb, wuvb, woutb, wuqb, wqrb, hrep, ybuf, yin, obuf,
                  lsem, usem, qsem, csend, crecv, gsend, grecv, rsend, rrecv, ysend, yrecv, osend, orecv):
    nx = ns // 2
    y, s = lax.axis_index("ctx"), lax.axis_index("seq")
    x, c = s // 2, s % 2
    rb, hb = y // 2, y % 2
    t_own, latent = cache.shape[1], cache.shape[2]
    rope_dim = rope.shape[1]
    nope = wuq.shape[3]
    d_model = hidden.shape[1]
    nh = wuk.shape[0]
    half_h = wuq.shape[2]
    nb = hidden.shape[0]
    half_b = nb // 2
    scale = (nope + rope_dim) ** -0.5
    n_pos = 2 * t_own
    cols = hidden.shape[1] // ns

    def at_y(d):
        return {"ctx": (y + d + ny) % ny, "seq": s}

    def at_x(d):
        return {"ctx": y, "seq": ((x + d + nx) % nx) * 2 + c}

    step = 256
    n_step = d_model // step
    r_step = 2
    group = 4
    uq = [pltpu.make_async_copy(wuq.at[pl.ds(k * step * group, step * group), hb], wuqb.at[pl.ds(k * step * group, step * group)], usem.at[k])
          for k in range(n_step // group)]
    qr = [pltpu.make_async_copy(wqr.at[pl.ds(hb * half_h + k * r_step, r_step)], wqrb.at[pl.ds(k * r_step, r_step)], qsem.at[k])
          for k in range(half_h // r_step)]
    span = pl.ds(c * t_own, t_own)
    local = [
        pltpu.make_async_copy(wuk.at[pl.ds(hb * half_h, half_h)], wukb, lsem.at[0]),
        pltpu.make_async_copy(cache, cacheb.at[:, span, pl.ds(0, latent)], lsem.at[1]),
        pltpu.make_async_copy(rope, ropeb.at[:, :, span], lsem.at[2]),
        pltpu.make_async_copy(wuv, wuvb, lsem.at[3]),
        pltpu.make_async_copy(wout, woutb, lsem.at[4]),
    ]
    loads = []
    for k in range(n_step // group):
        if k < half_h // r_step:
            loads.append((1, k, qr[k]))
        loads.append((0, k, uq[k]))
    in_flight = 5
    for _, _, copy in loads[:in_flight]:
        copy.start()

    barrier = pltpu.get_barrier_semaphore()
    for dy in range(ny):
        for ds in range(ns):
            if dy or ds:
                pl.semaphore_signal(barrier, inc=1, device_id={"ctx": (y + dy) % ny, "seq": (s + ds) % ns},
                                    device_id_type=MESH)

    wide_k = step * half_h
    si = lax.broadcasted_iota(jnp.int32, (2 * half_b, nb), 0)
    sj = lax.broadcasted_iota(jnp.int32, (2 * half_b, nb), 1)
    own_rows = jnp.where(sj == rb * half_b + si % half_b, 1.0, 0.0).astype(jnp.bfloat16)
    hid2 = jnp.dot(own_rows, hidden[...], preferred_element_type=jnp.float32).astype(jnp.bfloat16)
    stack = jnp.concatenate([hid2[:, step * k:step * k + step] for k in range(n_step)], axis=0)
    for n in range(half_h):
        ri = lax.broadcasted_iota(jnp.int32, (step, step), 0)
        rj = lax.broadcasted_iota(jnp.int32, (step, step), 1)
        spread = jnp.where(ri == (rj + n * step) // half_h, 1.0, 0.0).astype(jnp.bfloat16)
        hrep[:, n * step:(n + 1) * step] = jnp.dot(stack, spread, preferred_element_type=jnp.float32).astype(jnp.bfloat16)

    pl.semaphore_wait(barrier, ny * ns - 1)

    mate = {"ctx": y, "seq": s + 1 - 2 * c}
    other = pl.ds((1 - c) * t_own, t_own)
    swap = [
        pltpu.make_async_remote_copy(cache, cacheb.at[:, span, pl.ds(0, latent)], csend.at[0], crecv.at[0], device_id=mate, device_id_type=MESH),
        pltpu.make_async_remote_copy(rope, ropeb.at[:, :, span], csend.at[1], crecv.at[1], device_id=mate, device_id_type=MESH),
    ]
    q_rope = []
    lane_h = lax.broadcasted_iota(jnp.int32, (2 * half_b, wide_k), 1) % half_h
    row_h = lax.broadcasted_iota(jnp.int32, (2 * half_b, wide_k), 0) // half_b
    sums = [jnp.zeros((half_h * half_b, nope), jnp.float32) for _ in range(2)]
    for i, (kind, n, copy) in enumerate(loads):
        copy.wait()
        if i + in_flight < len(loads):
            loads[i + in_flight][2].start()
        else:
            k = i + in_flight - len(loads)
            if k < 3:
                local[k].start()
        if i == 5:
            for swap_copy in reversed(swap):
                swap_copy.start()
        if kind == 1:
            half = r_step * rope_dim // 2
            w = wqrb[n * r_step:(n + 1) * r_step].reshape(r_step * rope_dim, d_model)
            for p in range(2):
                q_rope.append(lax.dot_general(w[half * p:half * p + half], hid2, (((1,), (1,)), ((), ())), preferred_element_type=jnp.float32))
        else:
            for k in range(n * group, (n + 1) * group):
                hr = hrep[2 * half_b * k:2 * half_b * (k + 1), :]
                lhs = jnp.concatenate([jnp.where(lane_h == row_h + h, hr, jnp.zeros_like(hr)) for h in range(0, half_h, 2)], axis=0)
                w = wuqb[k * step:(k + 1) * step].reshape(wide_k, nope)
                sums[k % 2] = sums[k % 2] + jnp.dot(lhs, w, preferred_element_type=jnp.float32)
    q_rope = jnp.concatenate(q_rope, axis=0).T
    q_rope = jnp.concatenate([q_rope[0:half_b, rope_dim * h:rope_dim * (h + 1)] for h in range(half_h)], axis=0).astype(jnp.bfloat16)
    q_nope = (sums[0] + sums[1]).astype(jnp.bfloat16)

    n_q = half_b * half_h
    qi = lax.broadcasted_iota(jnp.int32, (n_q, n_q), 0)
    qj = lax.broadcasted_iota(jnp.int32, (n_q, n_q), 1)
    pick = jnp.where((qi % half_h == qj // half_b) & (qi // half_h == qj % half_b), 1.0, 0.0).astype(jnp.bfloat16)
    q_nope = jnp.dot(pick, q_nope, preferred_element_type=jnp.float32).astype(jnp.bfloat16)
    q_rope = jnp.dot(pick, q_rope, preferred_element_type=jnp.float32).astype(jnp.bfloat16)
    head_of = lax.broadcasted_iota(jnp.int32, (n_q, nope), 0) % half_h
    big = jnp.concatenate([jnp.where(head_of == h, q_nope, jnp.zeros_like(q_nope)) for h in range(half_h)], axis=1)
    local[0].wait()
    q_lat = jnp.dot(big, wukb[...].reshape(half_h * nope, latent), preferred_element_type=jnp.float32).astype(jnp.bfloat16)
    q_rope = jnp.concatenate([q_rope, jnp.zeros((n_q, LANES - rope_dim), jnp.bfloat16)], axis=1)
    for j in range(half_b // 2):
        qbuf[rb, j, hb, x, :, 0:latent] = q_lat[16 * j:16 * j + 16]
        qbuf[rb, j, hb, x, :, latent:] = q_rope[16 * j:16 * j + 16]

    sends = []

    def send(src, dst, ssem, rsem, to):
        copy = pltpu.make_async_remote_copy(src, dst, ssem, rsem, device_id=to, device_id_type=MESH)
        copy.start()
        sends.append(copy)

    def recv(dst, rsem):
        pltpu.make_async_remote_copy(dst, dst, rsem, rsem, device_id=mate, device_id_type=MESH).wait_recv()

    def rbhb(d):
        yy = (y + d + ny) % ny
        return yy // 2, yy % 2

    def xx(d):
        return (x + d + nx) % nx

    def cell(j, d1, d2):
        d_y, d_x = (d2, d1) if j < 2 else (d1, d2)
        r_, h_ = rbhb(-d_y)
        return qbuf.at[r_, j, h_, xx(-d_x)]

    def hop(j, stage, ref, along_x):
        for d in (2, 1, 3):
            send(ref, ref, gsend.at[j, stage, d], grecv.at[j, stage, d], at_x(d) if along_x else at_y(d))

    for a in range(2):
        for j in (a, a + 2):
            hop(j, 0, cell(j, 0, 0), j < 2)
        for j in (a, a + 2):
            hop(j, 1, cell(j, 0, 0), j >= 2)
    for a in range(2):
        for e in (1, 3, 2):
            for j in (a, a + 2):
                recv(cell(j, e, 0), grecv.at[j, 0, e])
                hop(j, 1 + e, cell(j, e, 0), j >= 2)

    def gather_finish(j):
        for e in range(4):
            for d in (1, 3, 2):
                recv(cell(j, e, d), grecv.at[j, 1 + e, d])

    for copy in local[3:]:
        copy.start()
    for copy in local[1:3]:
        copy.wait()
    recv(cacheb.at[:, other, pl.ds(0, latent)], crecv.at[0])
    recv(ropeb.at[:, :, other], crecv.at[1])
    for b in range(nb):
        keys = jnp.concatenate([ropeb[b], jnp.zeros((LANES - rope_dim, n_pos), jnp.bfloat16)], axis=0)
        cacheb[b, :, latent:] = keys.T
    gather_finish(0)
    gather_finish(2)

    base = (y * ns + 2 * x) * t_own
    n_head = qbuf.shape[2] * qbuf.shape[3] * 8
    lane = lax.broadcasted_iota(jnp.int32, (8, LANES), 1)
    n_slab = latent // LANES

    def stats(groups):
        tile = jnp.zeros((8, LANES), jnp.float32)
        for i, (m_, l_) in enumerate(groups):
            tile = jnp.where((lane >= 32 * i) & (lane < 32 * i + 16), m_, tile)
            tile = jnp.where((lane >= 32 * i + 16) & (lane < 32 * i + 32), l_, tile)
        return tile

    def attend(*pairs):
        first = lax.broadcasted_iota(jnp.int32, (n_pos, 2 * n_head), 1) % 16 < 8
        first_row = lax.broadcasted_iota(jnp.int32, (1, 2 * n_head), 1) % 16 < 8
        pos = lax.broadcasted_iota(jnp.int32, (n_pos, 2 * n_head), 0)
        b0s = [4 * r + 2 * (1 - cls) for cls, r in pairs]
        scores = []
        for (cls, r), b0 in zip(pairs, b0s):
            q2 = qbuf[r // 2, 1 - cls + 2 * (r % 2)].reshape(2 * n_head, qbuf.shape[5])
            scores.append([lax.dot_general(cacheb[b0 + i], q2, (((1,), (1,)), ((), ())), preferred_element_type=jnp.float32) for i in range(2)])
        res = []
        for sc, b0 in zip(scores, b0s):
            limit = jnp.where(first_row, lens[b0], lens[b0 + 1]) - base
            sc = jnp.where(first, sc[0], sc[1]) * scale
            sc = jnp.where(pos < limit, sc, NEG_FILL)
            m = jnp.maximum(jnp.max(sc, axis=0, keepdims=True), MAX_FLOOR)
            w = jnp.exp(sc - m)
            l = jnp.sum(w, axis=0, keepdims=True)
            res.append((m, l, w.astype(jnp.bfloat16).T))
        new = []
        for (m, l, w), b0 in zip(res, b0s):
            acc = [jnp.dot(w, cacheb[b0 + i, :, 0:latent], preferred_element_type=jnp.float32) for i in range(2)]
            new.append((acc, jnp.concatenate([m, l, jnp.zeros((6, 2 * n_head), jnp.float32)], axis=0).T))
        for (cls, r), (acc, ml_cols) in zip(pairs, new):
            for x_ in range(nx):
                ml = []
                for g in range(4):
                    k = ((g % 2) * nx + x_) * 16 + 8 * (g // 2)
                    ml.append((ml_cols[k:k + 8, 0:1], ml_cols[k:k + 8, 1:2]))
                    for n in range(n_slab):
                        part[cls, r, x_, 32 * n + 8 * g:32 * n + 8 * g + 8, :] = acc[g // 2][k:k + 8, LANES * n:LANES * n + LANES]
                part[cls, r, x_, 32 * n_slab:32 * n_slab + 8, :] = stats(ml)

    def merge(items):
        new = []
        row = 32 * n_slab
        for own, boxes in items:
            refs = [own] + boxes
            tiles = [ref[row:row + 8, :] for ref in refs]
            ml = []
            for g in range(4):
                ms = [jnp.broadcast_to(t[:, 32 * g:32 * g + 1], (8, LANES)) for t in tiles]
                ls = [jnp.broadcast_to(t[:, 32 * g + 16:32 * g + 17], (8, LANES)) for t in tiles]
                m = ms[0]
                for other_m in ms[1:]:
                    m = jnp.maximum(m, other_m)
                es = [jnp.exp(m_ - m) for m_ in ms]
                l = ls[0] * es[0]
                for l_, e_ in zip(ls[1:], es[1:]):
                    l = l + l_ * e_
                ml.append((m, l))
                for n in range(n_slab):
                    k = 32 * n + 8 * g
                    total = refs[0][k:k + 8, :] * es[0]
                    for ref, e_ in zip(refs[1:], es[1:]):
                        total = total + ref[k:k + 8, :] * e_
                    new.append((own, k, total))
            new.append((own, row, stats(ml)))
        for own, k, value in new:
            own[k:k + 8, :] = value

    def rs_send(cls, r, x_, i, to):
        send(part.at[cls, r, x_], inbox.at[cls, i], rsend.at[cls, i], rrecv.at[cls, i], to)

    def rs_merge(*items):
        for cls, _, _, slots in items:
            for i in slots:
                recv(inbox.at[cls, i], rrecv.at[cls, i])
        merge([(part.at[cls, r, x_], [inbox.at[cls, i] for i in slots]) for cls, r, x_, slots in items])

    def yy(d):
        return (y + d + ny) % ny

    def a_first(r):
        sg = 1 - 2 * (r % 2)
        rs_send(0, r, xx(2), r, at_x(sg))
        rs_send(0, r, xx(-sg), 4 + 2 * r + (1 + sg) // 2, at_x(-sg))

    def a_second(r):
        sg = 1 - 2 * (r % 2)
        rs_merge((0, r, xx(sg), [r]))
        rs_send(0, r, xx(sg), 4 + 2 * r + (1 - sg) // 2, at_x(sg))

    def b_send(d, odd):
        for x_ in range(odd, nx, 2):
            rs_send(1, yy(d), x_, 4 + 2 * x_ + (1 - d) // 2, at_y(d))

    def b_second(d, odd):
        rs_merge(*[(1, yy(d), x_, [x_]) for x_ in range(odd, nx, 2)])
        for x_ in range(odd, nx, 2):
            rs_send(1, yy(d), x_, 4 + 2 * x_ + (1 - d) // 2, at_y(d))

    def pair(r):
        return [4 + 2 * r, 5 + 2 * r]

    attend((1, yy(2)), (1, yy(1)))
    for x_ in range(nx):
        rs_send(1, yy(2), x_, x_, at_y(1 - 2 * (x_ % 2)))
    b_send(1, 1)
    gather_finish(1)
    gather_finish(3)
    attend((0, yy(2)), (1, yy(-1)))
    a_first(yy(2))
    b_send(-1, 0)
    attend((0, yy(1)), (0, yy(-1)))
    a_first(yy(1))
    a_first(yy(-1))
    attend((0, y), (1, y))
    a_first(y)
    b_second(1, 0)
    b_second(-1, 1)
    a_second(yy(2))
    a_second(yy(1))
    a_second(yy(-1))
    a_second(y)
    for d in (2, 1, 3):
        rs_merge((0, yy(d), x, pair(yy(d))), (1, y, xx(d), pair(xx(d))))
        rs_send(0, yy(d), x, 11 + d, at_y(d))
        rs_send(1, y, xx(d), 11 + d, at_x(d))
    rs_merge((0, y, x, pair(y)), (1, y, x, pair(x)))
    rs_merge((0, y, x, [12, 13, 14]), (1, y, x, [12, 13, 14]))

    rows = []
    for cls in (1, 0):
        own = part.at[cls, y, x]
        st = own[32 * n_slab:32 * n_slab + 8, :]
        for g in range(4):
            inv = jnp.broadcast_to(st[:, 32 * g + 16:32 * g + 17], (8, LANES))
            rows.append(jnp.concatenate([own[32 * n + 8 * g:32 * n + 8 * g + 8, :] / inv for n in range(n_slab)], axis=1))
    o_l = jnp.concatenate(rows, axis=0).astype(jnp.bfloat16)
    n_own = o_l.shape[0]
    local[3].wait()
    head_o = lax.broadcasted_iota(jnp.int32, (n_own, wuv.shape[2]), 0) % nh
    v = jnp.zeros((n_own, wuv.shape[2]), jnp.float32)
    for h in range(nh):
        v = jnp.where(head_o == h, jnp.dot(o_l, wuvb[h], preferred_element_type=jnp.float32), v)
    v = v.astype(jnp.bfloat16)
    pi = lax.broadcasted_iota(jnp.int32, (16 * nh, n_own), 0)
    pj = lax.broadcasted_iota(jnp.int32, (16 * nh, n_own), 1)
    perm = jnp.where((pj % nh == pi // 16) & (pj // nh == pi % 16), 1.0, 0.0).astype(jnp.bfloat16)
    vp = jnp.dot(perm, v, preferred_element_type=jnp.float32).astype(jnp.bfloat16)
    lhs = jnp.concatenate([vp[16 * h:16 * h + 16] for h in range(nh)], axis=1)
    local[4].wait()
    n_rows = n_own // nh
    others = [(d, f) for d in (2, 1, 3, 0) for f in (0, 1) if (d, f) != (0, 0)]
    for d, f in others + [(0, 0)]:
        s_ = xx(d) * 2 + (1 - c if f else c)
        piece = jnp.dot(lhs, woutb[:, pl.ds(pl.multiple_of(s_ * cols, LANES), cols)], preferred_element_type=jnp.float32)
        if (d, f) != (0, 0):
            k = 2 * d + f
            k_there = 2 * ((nx - d) % nx) + f
            ybuf[k] = piece[0:n_rows]
            send(ybuf.at[k], yin.at[k_there], ysend.at[k], yrecv.at[k_there], {"ctx": y, "seq": s_})
        else:
            total = piece[0:n_rows]
    for d, f in others:
        recv(yin.at[2 * d + f], yrecv.at[2 * d + f])
        total = total + yin[2 * d + f]
    hid = hidden[:, pl.ds(pl.multiple_of(s * cols, LANES), cols)].astype(jnp.float32)
    mine = hid[0:n_rows]
    for y_ in range(1, ny):
        mine = jnp.where(y == y_, hid[n_rows * y_:n_rows * y_ + n_rows], mine)
    obuf[y * ns + s] = (mine + total).astype(jnp.bfloat16)
    me = y * ns + s
    far = [(e, d, f) for e in (2, 1, 3, 0) for d in (2, 1, 3, 0) for f in (0, 1) if (e, d, f) != (0, 0, 0)]
    far.sort(key=lambda t: -(min(t[0], ny - t[0]) + min(t[1], nx - t[1])))
    for e, d, f in far:
        k = (e * nx + d) * 2 + f
        send(obuf.at[me], obuf.at[me], osend.at[k], orecv.at[k], {"ctx": yy(e), "seq": xx(d) * 2 + (1 - c if f else c)})
    for e, d, f in reversed(far):
        recv(obuf.at[yy(-e) * ns + xx(-d) * 2 + (1 - c if f else c)], orecv.at[(e * nx + d) * 2 + f])
    for s_ in range(ns):
        out[:, s_ * cols:(s_ + 1) * cols] = jnp.concatenate(
            [obuf[y_ * ns + s_].astype(jnp.float32) for y_ in range(ny)], axis=0).astype(jnp.bfloat16)
    for copy in sends:
        copy.wait_send()
    for copy in swap:
        copy.wait_send()


def solution(mesh):
    ny, ns = mesh.shape['ctx'], mesh.shape['seq']
    row_spec = P('batch', None)
    cache_spec = P('batch', ('ctx', 'seq'), None)
    proj_spec = P(None, 'seq', None)
    head_spec = P('seq', None, None)

    def local_step(hidden, lengths, latent_cache, rope_keys, w_uq, w_qr, w_uk, w_uv, w_out):
        rope_t = jnp.transpose(rope_keys, (0, 2, 1))
        nb, d_model = hidden.shape
        t_own, latent = latent_cache.shape[1:]
        nh = w_uq.shape[1]
        wqr_t = jnp.transpose(w_qr, (1, 2, 0))
        rope_dim = rope_t.shape[1]
        nx = ns // 2
        cols = d_model // ns
        n_rows = nb // ny
        bf, f32 = jnp.bfloat16, jnp.float32
        unit = (latent // LANES) * 32 + 8
        wide = latent + LANES
        dma = pltpu.SemaphoreType.DMA
        vmem = pl.BlockSpec(memory_space=pltpu.VMEM)
        anyw = pl.BlockSpec(memory_space=pl.ANY)
        import functools
        out = pl.pallas_call(
            functools.partial(decode_kernel, ny, ns),
            out_shape=jax.ShapeDtypeStruct(hidden.shape, bf),
            in_specs=[pl.BlockSpec(memory_space=pltpu.SMEM), vmem, anyw, anyw, anyw, anyw, anyw, anyw, anyw],
            out_specs=vmem,
            scratch_shapes=[
                pltpu.VMEM((nb, 2 * t_own, wide), bf),
                pltpu.VMEM((nb, rope_dim, 2 * t_own), bf),
                pltpu.VMEM((2, nb // 4, 2, nx, 16, wide), bf),
                pltpu.VMEM((2, ny, nx, unit, LANES), f32),
                pltpu.VMEM((2, 15, unit, LANES), f32),
                pltpu.VMEM((nh // 2,) + w_uk.shape[1:], bf),
                pltpu.VMEM(w_uv.shape, bf),
                pltpu.VMEM((w_out.shape[0] * w_out.shape[1], d_model), bf),
                pltpu.VMEM((d_model, nh // 2, w_uq.shape[2]), bf),
                pltpu.VMEM((nh // 2, rope_dim, d_model), bf),
                pltpu.VMEM((d_model // 256 * 16, 256 * nh // 2), bf),
                pltpu.VMEM((ns, n_rows, cols), f32),
                pltpu.VMEM((ns, n_rows, cols), f32),
                pltpu.VMEM((ny * ns, n_rows, cols), bf),
                dma((5,)), dma((d_model // 256,)), dma((nh // 4,)), dma((2,)), dma((2,)), dma((4, 5, 4)), dma((4, 5, 4)), dma((2, 15)), dma((2, 15)),
                dma((ns,)), dma((ns,)), dma((ny * ns,)), dma((ny * ns,)),
            ],
            compiler_params=pltpu.CompilerParams(collective_id=0, has_side_effects=True, vmem_limit_bytes=60 * 2 ** 20),
        )(lengths, hidden, w_uq.reshape(d_model, 2, nh // 2, -1), wqr_t, w_uk, latent_cache, rope_t, w_uv, w_out.reshape(-1, d_model))
        return out

    return jax.shard_map(local_step, mesh=mesh,
                         in_specs=(row_spec, P('batch'), cache_spec, cache_spec, proj_spec, proj_spec, head_spec, head_spec, head_spec),
                         out_specs=row_spec, check_vma=False)
```

```python
import jax
import jax.numpy as jnp
from jax import lax
from jax.experimental import pallas as pl
from jax.experimental.pallas import tpu as pltpu
from jax.sharding import PartitionSpec as P

NEG_FILL = -3.0e38
MAX_FLOOR = -1.5e38
LANES = 128
MESH = pl.DeviceIdType.MESH


def decode_kernel(ny, ns, lens_in, hidden_in, wuq, wqr, wuk, cache, rope, wuv, wout, out,
                  lens, hidden, cacheb, ropeb, qbuf, part, inbox, wukb, wuvb, woutb, wuqb, wqrb, hrep, ybuf, yin, obuf,
                  lsem, usem, qsem, csend, crecv, gsend, grecv, rsend, rrecv, tail_sem):
    nx = ns // 2
    y, s = lax.axis_index("ctx"), lax.axis_index("seq")
    x, c = s // 2, s % 2
    rb, hb = y // 2, y % 2
    t_own, latent = cache.shape[1], cache.shape[2]
    rope_dim = rope.shape[1]
    nope = wuq.shape[3]
    d_model = hidden.shape[1]
    nh = wuk.shape[0]
    half_h = wuq.shape[2]
    nb = hidden.shape[0]
    half_b = nb // 2
    scale = (nope + rope_dim) ** -0.5
    n_pos = 2 * t_own
    cols = hidden.shape[1] // ns

    def at_y(d):
        return {"ctx": (y + d + ny) % ny, "seq": s}

    def at_x(d):
        return {"ctx": y, "seq": ((x + d + nx) % nx) * 2 + c}

    step = 256
    n_step = d_model // step
    r_step = 2
    group = 4
    uq = [pltpu.make_async_copy(wuq.at[pl.ds(k * step * group, step * group), hb], wuqb.at[pl.ds(k * step * group, step * group)], usem.at[k])
          for k in range(n_step // group)]
    qr = [pltpu.make_async_copy(wqr.at[pl.ds(hb * half_h + k * r_step, r_step)], wqrb.at[pl.ds(k * r_step, r_step)], qsem.at[k])
          for k in range(half_h // r_step)]
    span = pl.ds(c * t_own, t_own)
    local = [
        pltpu.make_async_copy(wuk.at[pl.ds(hb * half_h, half_h)], wukb, lsem.at[0]),
        pltpu.make_async_copy(cache, cacheb.at[:, span, pl.ds(0, latent)], lsem.at[1]),
        pltpu.make_async_copy(rope, ropeb.at[:, :, span], lsem.at[2]),
        pltpu.make_async_copy(wuv, wuvb, lsem.at[3]),
        pltpu.make_async_copy(wout, woutb, lsem.at[4]),
    ]
    loads = []
    for k in range(n_step // group):
        if k < half_h // r_step:
            loads.append((1, k, qr[k]))
        loads.append((0, k, uq[k]))
    in_flight = 5
    small = [pltpu.make_async_copy(hidden_in, hidden, lsem.at[5]), pltpu.make_async_copy(lens_in, lens, lsem.at[6])]
    for copy in small:
        copy.start()
    for _, _, copy in loads[:in_flight]:
        copy.start()

    barrier = pltpu.get_barrier_semaphore()
    for dy in range(ny):
        for ds in range(ns):
            if dy or ds:
                pl.semaphore_signal(barrier, inc=1, device_id={"ctx": (y + dy) % ny, "seq": (s + ds) % ns},
                                    device_id_type=MESH)

    for copy in small:
        copy.wait()
    wide_k = step * half_h
    si = lax.broadcasted_iota(jnp.int32, (2 * half_b, nb), 0)
    sj = lax.broadcasted_iota(jnp.int32, (2 * half_b, nb), 1)
    own_rows = jnp.where(sj == rb * half_b + si % half_b, 1.0, 0.0).astype(jnp.bfloat16)
    hid2 = jnp.dot(own_rows, hidden[...], preferred_element_type=jnp.float32).astype(jnp.bfloat16)
    stack = jnp.concatenate([hid2[:, step * k:step * k + step] for k in range(n_step)], axis=0)
    for n in range(half_h):
        ri = lax.broadcasted_iota(jnp.int32, (step, step), 0)
        rj = lax.broadcasted_iota(jnp.int32, (step, step), 1)
        spread = jnp.where(ri == (rj + n * step) // half_h, 1.0, 0.0).astype(jnp.bfloat16)
        hrep[:, n * step:(n + 1) * step] = jnp.dot(stack, spread, preferred_element_type=jnp.float32).astype(jnp.bfloat16)

    pl.semaphore_wait(barrier, ny * ns - 1)

    mate = {"ctx": y, "seq": s + 1 - 2 * c}
    other = pl.ds((1 - c) * t_own, t_own)
    swap = [
        pltpu.make_async_remote_copy(cache, cacheb.at[:, span, pl.ds(0, latent)], csend.at[0], crecv.at[0], device_id=mate, device_id_type=MESH),
        pltpu.make_async_remote_copy(rope, ropeb.at[:, :, span], csend.at[1], crecv.at[1], device_id=mate, device_id_type=MESH),
    ]
    q_rope = []
    lane_h = lax.broadcasted_iota(jnp.int32, (2 * half_b, wide_k), 1) % half_h
    row_h = lax.broadcasted_iota(jnp.int32, (2 * half_b, wide_k), 0) // half_b
    sums = [jnp.zeros((half_h * half_b, nope), jnp.float32) for _ in range(2)]
    for i, (kind, n, copy) in enumerate(loads):
        copy.wait()
        if i + in_flight < len(loads):
            loads[i + in_flight][2].start()
        else:
            k = i + in_flight - len(loads)
            if k < 3:
                local[k].start()
        if i == 5:
            for swap_copy in reversed(swap):
                swap_copy.start()
        if kind == 1:
            half = r_step * rope_dim // 2
            w = wqrb[n * r_step:(n + 1) * r_step].reshape(r_step * rope_dim, d_model)
            for p in range(2):
                q_rope.append(lax.dot_general(w[half * p:half * p + half], hid2, (((1,), (1,)), ((), ())), preferred_element_type=jnp.float32))
        else:
            for k in range(n * group, (n + 1) * group):
                hr = hrep[2 * half_b * k:2 * half_b * (k + 1), :]
                lhs = jnp.concatenate([jnp.where(lane_h == row_h + h, hr, jnp.zeros_like(hr)) for h in range(0, half_h, 2)], axis=0)
                w = wuqb[k * step:(k + 1) * step].reshape(wide_k, nope)
                sums[k % 2] = sums[k % 2] + jnp.dot(lhs, w, preferred_element_type=jnp.float32)
    q_rope = jnp.concatenate(q_rope, axis=0).T
    q_rope = jnp.concatenate([q_rope[0:half_b, rope_dim * h:rope_dim * (h + 1)] for h in range(half_h)], axis=0).astype(jnp.bfloat16)
    q_nope = (sums[0] + sums[1]).astype(jnp.bfloat16)

    n_q = half_b * half_h
    qi = lax.broadcasted_iota(jnp.int32, (n_q, n_q), 0)
    qj = lax.broadcasted_iota(jnp.int32, (n_q, n_q), 1)
    pick = jnp.where((qi % half_h == qj // half_b) & (qi // half_h == qj % half_b), 1.0, 0.0).astype(jnp.bfloat16)
    q_nope = jnp.dot(pick, q_nope, preferred_element_type=jnp.float32).astype(jnp.bfloat16)
    q_rope = jnp.dot(pick, q_rope, preferred_element_type=jnp.float32)
    head_of = lax.broadcasted_iota(jnp.int32, (n_q, nope), 0) % half_h
    big = jnp.concatenate([jnp.where(head_of == h, q_nope, jnp.zeros_like(q_nope)) for h in range(half_h)], axis=1)
    local[0].wait()
    q_lat = jnp.dot(big, wukb[...].reshape(half_h * nope, latent), preferred_element_type=jnp.float32).astype(jnp.bfloat16)
    for j in range(half_b // 2):
        for n in range(latent // LANES):
            qbuf[rb, j, hb, x, 16 * n:16 * n + 16, :] = q_lat[16 * j:16 * j + 16, LANES * n:LANES * n + LANES]
        sides = [q_rope[16 * j + 8 * i:16 * j + 8 * i + 8] for i in range(2)]
        qbuf[rb, j, hb, x, 64:72, :] = jnp.concatenate(sides, axis=1).astype(jnp.bfloat16)


    def send(src, dst, ssem, rsem, to):
        copy = pltpu.make_async_remote_copy(src, dst, ssem, rsem, device_id=to, device_id_type=MESH)
        copy.start()

    def recv(dst, rsem):
        pltpu.make_async_remote_copy(dst, dst, rsem, rsem, device_id=mate, device_id_type=MESH).wait_recv()

    def sent(src, ssem):
        pltpu.make_async_remote_copy(src, src, ssem, ssem, device_id=mate, device_id_type=MESH).wait_send()

    def rbhb(d):
        yy = (y + d + ny) % ny
        return yy // 2, yy % 2

    def xx(d):
        return (x + d + nx) % nx

    def cell(j, d1, d2):
        d_y, d_x = (d2, d1) if j < 2 else (d1, d2)
        r_, h_ = rbhb(-d_y)
        return qbuf.at[r_, j, h_, xx(-d_x)]

    def hop(j, stage, ref, along_x):
        for d in (2, 1, 3):
            send(ref, ref, gsend.at[1 if stage else 0], grecv.at[j, 0 if stage else d], at_x(d) if along_x else at_y(d))

    for a in range(2):
        for j in (a, a + 2):
            hop(j, 0, cell(j, 0, 0), j < 2)
        for j in (a, a + 2):
            hop(j, 1, cell(j, 0, 0), j >= 2)
    for a in range(2):
        for e in (1, 3, 2):
            for j in (a, a + 2):
                recv(cell(j, e, 0), grecv.at[j, e])
                hop(j, 1 + e, cell(j, e, 0), j >= 2)

    def gather_finish(j):
        recv(qbuf.at[0, 0:3, 0], grecv.at[j, 0])

    for copy in local[3:]:
        copy.start()
    for copy in local[1:3]:
        copy.wait()
    recv(cacheb.at[:, other, pl.ds(0, latent)], crecv.at[0])
    recv(ropeb.at[:, :, other], crecv.at[1])
    for b in range(nb):
        blank = jnp.zeros((LANES - rope_dim, n_pos), jnp.bfloat16)
        keys = jnp.concatenate([blank, ropeb[b]] if b % 2 else [ropeb[b], blank], axis=0)
        cacheb[b, :, latent:] = keys.T
    gather_finish(0)
    gather_finish(2)

    base = (y * ns + 2 * x) * t_own
    n_head = qbuf.shape[2] * qbuf.shape[3] * 8
    lane = lax.broadcasted_iota(jnp.int32, (8, LANES), 1)
    n_slab = latent // LANES

    def stats(groups):
        tile = jnp.zeros((8, LANES), jnp.float32)
        for i, (m_, l_) in enumerate(groups):
            tile = jnp.where((lane >= 32 * i) & (lane < 32 * i + 16), m_, tile)
            tile = jnp.where((lane >= 32 * i + 16) & (lane < 32 * i + 32), l_, tile)
        return tile

    def attend(*pairs):
        first = lax.broadcasted_iota(jnp.int32, (n_pos, 2 * n_head), 1) % 16 < 8
        first_row = lax.broadcasted_iota(jnp.int32, (1, 2 * n_head), 1) % 16 < 8
        pos = lax.broadcasted_iota(jnp.int32, (n_pos, 2 * n_head), 0)
        b0s = [4 * r + 2 * (1 - cls) for cls, r in pairs]
        scores = []
        for (cls, r), b0 in zip(pairs, b0s):
            r_, j_ = r // 2, 1 - cls + 2 * (r % 2)
            slabs = [qbuf[r_, j_, :, :, 16 * n:16 * n + 16, :].reshape(2 * n_head, LANES) for n in range(n_slab)]
            side = qbuf[r_, j_, :, :, 64:72, :]
            side = jnp.concatenate([side, side], axis=2).reshape(2 * n_head, LANES)
            q2 = jnp.concatenate(slabs + [side], axis=1)
            scores.append([lax.dot_general(cacheb[b0 + i], q2, (((1,), (1,)), ((), ())), preferred_element_type=jnp.float32) for i in range(2)])
        res = []
        for sc, b0 in zip(scores, b0s):
            limit = jnp.where(first_row, lens[b0], lens[b0 + 1]) - base
            sc = jnp.where(first, sc[0], sc[1]) * scale
            sc = jnp.where(pos < limit, sc, NEG_FILL)
            m = jnp.maximum(jnp.max(sc, axis=0, keepdims=True), MAX_FLOOR)
            w = jnp.exp(sc - m)
            l = jnp.sum(w, axis=0, keepdims=True)
            res.append((m, l, w.astype(jnp.bfloat16).T))
        new = []
        for (m, l, w), b0 in zip(res, b0s):
            acc = [jnp.dot(w, cacheb[b0 + i, :, 0:latent], preferred_element_type=jnp.float32) for i in range(2)]
            new.append((acc, jnp.concatenate([m, l, jnp.zeros((6, 2 * n_head), jnp.float32)], axis=0).T))
        for (cls, r), (acc, ml_cols) in zip(pairs, new):
            for x_ in range(nx):
                ml = []
                for g in range(4):
                    k = ((g % 2) * nx + x_) * 16 + 8 * (g // 2)
                    ml.append((ml_cols[k:k + 8, 0:1], ml_cols[k:k + 8, 1:2]))
                    for n in range(n_slab):
                        part[cls, r, x_, 32 * n + 8 * g:32 * n + 8 * g + 8, :] = acc[g // 2][k:k + 8, LANES * n:LANES * n + LANES]
                part[cls, r, x_, 32 * n_slab:32 * n_slab + 8, :] = stats(ml)

    def merge(items):
        new = []
        row = 32 * n_slab
        for own, boxes in items:
            refs = [own] + boxes
            tiles = [ref[row:row + 8, :] for ref in refs]
            ml = []
            for g in range(4):
                ms = [jnp.broadcast_to(t[:, 32 * g:32 * g + 1], (8, LANES)) for t in tiles]
                ls = [jnp.broadcast_to(t[:, 32 * g + 16:32 * g + 17], (8, LANES)) for t in tiles]
                m = ms[0]
                for other_m in ms[1:]:
                    m = jnp.maximum(m, other_m)
                es = [jnp.exp(m_ - m) for m_ in ms]
                l = ls[0] * es[0]
                for l_, e_ in zip(ls[1:], es[1:]):
                    l = l + l_ * e_
                ml.append((m, l))
                for n in range(n_slab):
                    k = 32 * n + 8 * g
                    total = refs[0][k:k + 8, :] * es[0]
                    for ref, e_ in zip(refs[1:], es[1:]):
                        total = total + ref[k:k + 8, :] * e_
                    new.append((own, k, total))
            new.append((own, row, stats(ml)))
        for own, k, value in new:
            own[k:k + 8, :] = value

    def rs_send(cls, r, x_, i, sem, to):
        send(part.at[cls, r, x_], inbox.at[cls, i], rsend.at[0], rrecv.at[cls, sem], to)

    def rs_merge(*items):
        for cls, _, _, i, n, sem in items:
            recv(inbox.at[cls, pl.ds(i, n)], rrecv.at[cls, sem])
        merge([(part.at[cls, r, x_], [inbox.at[cls, i + k] for k in range(n)]) for cls, r, x_, i, n, _ in items])

    def yy(d):
        return (y + d + ny) % ny

    def a_first(r):
        sg = 1 - 2 * (r % 2)
        rs_send(0, r, xx(2), r, r, at_x(sg))
        rs_send(0, r, xx(-sg), 4 + 2 * r + (1 + sg) // 2, 4 + r, at_x(-sg))

    def a_second(r):
        sg = 1 - 2 * (r % 2)
        rs_merge((0, r, xx(sg), r, 1, r))
        rs_send(0, r, xx(sg), 4 + 2 * r + (1 - sg) // 2, 4 + r, at_x(sg))

    def b_send(d, odd):
        for x_ in range(odd, nx, 2):
            rs_send(1, yy(d), x_, 4 + 2 * x_ + (1 - d) // 2, 4 + x_, at_y(d))

    def b_second(d, odd):
        rs_merge(*[(1, yy(d), x_, x_, 1, x_) for x_ in range(odd, nx, 2)])
        for x_ in range(odd, nx, 2):
            rs_send(1, yy(d), x_, 4 + 2 * x_ + (1 - d) // 2, 4 + x_, at_y(d))

    def pair(cls, r, x_, k):
        return (cls, r, x_, 4 + 2 * k, 2, 4 + k)

    attend((1, yy(2)), (1, yy(1)))
    for x_ in range(nx):
        rs_send(1, yy(2), x_, x_, x_, at_y(1 - 2 * (x_ % 2)))
    b_send(1, 1)
    gather_finish(1)
    gather_finish(3)
    attend((0, yy(2)), (1, yy(-1)))
    a_first(yy(2))
    b_send(-1, 0)
    attend((0, yy(1)), (0, yy(-1)))
    a_first(yy(1))
    a_first(yy(-1))
    attend((0, y), (1, y))
    a_first(y)
    b_second(1, 0)
    b_second(-1, 1)
    a_second(yy(2))
    a_second(yy(1))
    a_second(yy(-1))
    a_second(y)
    for d in (2, 1, 3):
        rs_merge(pair(0, yy(d), x, yy(d)), pair(1, y, xx(d), xx(d)))
        rs_send(0, yy(d), x, 11 + d, 8, at_y(d))
        rs_send(1, y, xx(d), 11 + d, 8, at_x(d))
    rs_merge(pair(0, y, x, y), pair(1, y, x, x))
    rs_merge((0, y, x, 12, 3, 8), (1, y, x, 12, 3, 8))

    rows = []
    for cls in (1, 0):
        own = part.at[cls, y, x]
        st = own[32 * n_slab:32 * n_slab + 8, :]
        for g in range(4):
            inv = jnp.broadcast_to(st[:, 32 * g + 16:32 * g + 17], (8, LANES))
            rows.append(jnp.concatenate([own[32 * n + 8 * g:32 * n + 8 * g + 8, :] / inv for n in range(n_slab)], axis=1))
    o_l = jnp.concatenate(rows, axis=0).astype(jnp.bfloat16)
    n_own = o_l.shape[0]
    local[3].wait()
    head_o = lax.broadcasted_iota(jnp.int32, (n_own, wuv.shape[2]), 0) % nh
    v = jnp.zeros((n_own, wuv.shape[2]), jnp.float32)
    for h in range(nh):
        v = jnp.where(head_o == h, jnp.dot(o_l, wuvb[h], preferred_element_type=jnp.float32), v)
    v = v.astype(jnp.bfloat16)
    pi = lax.broadcasted_iota(jnp.int32, (16 * nh, n_own), 0)
    pj = lax.broadcasted_iota(jnp.int32, (16 * nh, n_own), 1)
    perm = jnp.where((pj % nh == pi // 16) & (pj // nh == pi % 16), 1.0, 0.0).astype(jnp.bfloat16)
    vp = jnp.dot(perm, v, preferred_element_type=jnp.float32).astype(jnp.bfloat16)
    lhs = jnp.concatenate([vp[16 * h:16 * h + 16] for h in range(nh)], axis=1)
    local[4].wait()
    n_rows = n_own // nh
    others = [(d, f) for d in (2, 1, 3, 0) for f in (0, 1) if (d, f) != (0, 0)]
    for d, f in others + [(0, 0)]:
        s_ = xx(d) * 2 + (1 - c if f else c)
        piece = jnp.dot(lhs, woutb[:, pl.ds(pl.multiple_of(s_ * cols, LANES), cols)], preferred_element_type=jnp.float32)
        if (d, f) != (0, 0):
            k = 2 * d + f
            k_there = 2 * ((nx - d) % nx) + f
            ybuf[k] = piece[0:n_rows]
            send(ybuf.at[k], yin.at[k_there], tail_sem.at[0], tail_sem.at[1], {"ctx": y, "seq": s_})
        else:
            total = piece[0:n_rows]
    recv(yin.at[1:ns], tail_sem.at[1])
    for d, f in others:
        total = total + yin[2 * d + f]
    hid = hidden[:, pl.ds(pl.multiple_of(s * cols, LANES), cols)].astype(jnp.float32)
    mine = hid[0:n_rows]
    for y_ in range(1, ny):
        mine = jnp.where(y == y_, hid[n_rows * y_:n_rows * y_ + n_rows], mine)
    obuf[y * ns + s] = (mine + total).astype(jnp.bfloat16)
    me = y * ns + s
    far = [(e, d, f) for e in (2, 1, 3, 0) for d in (2, 1, 3, 0) for f in (0, 1) if (e, d, f) != (0, 0, 0)]
    far.sort(key=lambda t: -(min(t[0], ny - t[0]) + min(t[1], nx - t[1])))
    for e, d, f in far:
        send(obuf.at[me], obuf.at[me], tail_sem.at[2], tail_sem.at[3], {"ctx": yy(e), "seq": xx(d) * 2 + (1 - c if f else c)})
    recv(obuf.at[1:ny * ns], tail_sem.at[3])
    for s_ in range(ns):
        out[:, s_ * cols:(s_ + 1) * cols] = jnp.concatenate(
            [obuf[y_ * ns + s_].astype(jnp.float32) for y_ in range(ny)], axis=0).astype(jnp.bfloat16)
    sent(qbuf.at[0, 0:3, 0], gsend.at[0])
    sent(qbuf.at[:, 0:3], gsend.at[1])
    sent(inbox, rsend.at[0])
    sent(ybuf.at[1:ns], tail_sem.at[0])
    sent(obuf.at[1:ny * ns], tail_sem.at[2])
    for copy in swap:
        copy.wait_send()


def solution(mesh):
    ny, ns = mesh.shape['ctx'], mesh.shape['seq']
    row_spec = P('batch', None)
    cache_spec = P('batch', ('ctx', 'seq'), None)
    proj_spec = P(None, 'seq', None)
    head_spec = P('seq', None, None)

    def local_step(hidden, lengths, latent_cache, rope_keys, w_uq, w_qr, w_uk, w_uv, w_out):
        rope_t = jnp.transpose(rope_keys, (0, 2, 1))
        nb, d_model = hidden.shape
        t_own, latent = latent_cache.shape[1:]
        nh = w_uq.shape[1]
        wqr_t = jnp.transpose(w_qr, (1, 2, 0))
        rope_dim = rope_t.shape[1]
        nx = ns // 2
        cols = d_model // ns
        n_rows = nb // ny
        bf, f32 = jnp.bfloat16, jnp.float32
        unit = (latent // LANES) * 32 + 8
        wide = latent + LANES
        dma = pltpu.SemaphoreType.DMA
        vmem = pl.BlockSpec(memory_space=pltpu.VMEM)
        anyw = pl.BlockSpec(memory_space=pl.ANY)
        import functools
        out = pl.pallas_call(
            functools.partial(decode_kernel, ny, ns),
            out_shape=pltpu.VMEM(hidden.shape, bf),
            in_specs=[anyw, anyw, anyw, anyw, anyw, anyw, anyw, anyw, anyw],
            out_specs=vmem,
            scratch_shapes=[
                pltpu.SMEM(lengths.shape, jnp.int32),
                pltpu.VMEM(hidden.shape, bf),
                pltpu.VMEM((nb, 2 * t_own, wide), bf),
                pltpu.VMEM((nb, rope_dim, 2 * t_own), bf),
                pltpu.VMEM((2, nb // 4, 2, nx, latent // 8 + 8, LANES), bf),
                pltpu.VMEM((2, ny, nx, unit, LANES), f32),
                pltpu.VMEM((2, 15, unit, LANES), f32),
                pltpu.VMEM((nh // 2,) + w_uk.shape[1:], bf),
                pltpu.VMEM(w_uv.shape, bf),
                pltpu.VMEM((w_out.shape[0] * w_out.shape[1], d_model), bf),
                pltpu.VMEM((d_model, nh // 2, w_uq.shape[2]), bf),
                pltpu.VMEM((nh // 2, rope_dim, d_model), bf),
                pltpu.VMEM((d_model // 256 * 16, 256 * nh // 2), bf),
                pltpu.VMEM((ns, n_rows, cols), f32),
                pltpu.VMEM((ns, n_rows, cols), f32),
                pltpu.VMEM((ny * ns, n_rows, cols), bf),
                dma((7,)), dma((d_model // 256,)), dma((nh // 4,)), dma((2,)), dma((2,)), dma((2,)), dma((4, 4)), dma((1,)), dma((2, 9)),
                dma((4,)),
            ],
            compiler_params=pltpu.CompilerParams(collective_id=0, has_side_effects=True, vmem_limit_bytes=60 * 2 ** 20),
        )(lengths, hidden, w_uq.reshape(d_model, 2, nh // 2, -1), wqr_t, w_uk, latent_cache, rope_t, w_uv, w_out.reshape(-1, d_model))
        return out

    return jax.shard_map(local_step, mesh=mesh,
                         in_specs=(row_spec, P('batch'), cache_spec, cache_spec, proj_spec, proj_spec, head_spec, head_spec, head_spec),
                         out_specs=row_spec, check_vma=False)
```

```python
import jax
import jax.numpy as jnp
from jax import lax
from jax.experimental import pallas as pl
from jax.experimental.pallas import tpu as pltpu
from jax.sharding import PartitionSpec as P

NEG_FILL = -3.0e38
MAX_FLOOR = -1.5e38
LANES = 128
MESH = pl.DeviceIdType.MESH
SUB = 8
UNIT = 32
PACK = 16
OTHERS = (2, 1, 3)


def block(i, n):
    return slice(i * n, (i + 1) * n)


def decode_kernel(ny, ns, lens_in, hidden_in, wuq, wqr, wuk, cache, rope, wuv, wout, out,
                  lens, hidden, cacheb, ropeb, qbuf, part, inbox, wukb, wuvb, woutb, wuqb, wqrb, hrep, ybuf, yin, obuf,
                  lsem, usem, qsem, csend, crecv, gsend, grecv, rsend, rrecv, tail_sem):
    nx = ns // 2
    y, s = lax.axis_index("ctx"), lax.axis_index("seq")
    x, c = s // 2, s % 2
    rb, hb = y // 2, y % 2
    t_own, latent = cache.shape[1], cache.shape[2]
    rope_dim = rope.shape[1]
    nope = wuq.shape[3]
    d_model = hidden.shape[1]
    nh = wuk.shape[0]
    half_h = wuq.shape[2]
    nb = hidden.shape[0]
    half_b = nb // 2
    scale = (nope + rope_dim) ** -0.5
    n_pos = 2 * t_own
    cols = hidden.shape[1] // ns

    def at_y(d):
        return {"ctx": (y + d + ny) % ny, "seq": s}

    def at_x(d):
        return {"ctx": y, "seq": ((x + d + nx) % nx) * 2 + c}

    step = 256
    n_step = d_model // step
    r_step = 2
    group = 4
    uq = [pltpu.make_async_copy(wuq.at[pl.ds(k * step * group, step * group), hb], wuqb.at[pl.ds(k * step * group, step * group)], usem.at[k])
          for k in range(n_step // group)]
    qr = [pltpu.make_async_copy(wqr.at[pl.ds(hb * half_h + k * r_step, r_step)], wqrb.at[pl.ds(k * r_step, r_step)], qsem.at[k])
          for k in range(half_h // r_step)]
    span = pl.ds(c * t_own, t_own)
    local = [
        pltpu.make_async_copy(wuk.at[pl.ds(hb * half_h, half_h)], wukb, lsem.at[0]),
        pltpu.make_async_copy(cache, cacheb.at[:, span, pl.ds(0, latent)], lsem.at[1]),
        pltpu.make_async_copy(rope, ropeb.at[:, :, span], lsem.at[2]),
        pltpu.make_async_copy(wuv, wuvb, lsem.at[3]),
        pltpu.make_async_copy(wout, woutb, lsem.at[4]),
    ]
    loads = []
    for k in range(n_step // group):
        if k < half_h // r_step:
            loads.append((1, k, qr[k]))
        loads.append((0, k, uq[k]))
    in_flight = 5
    small = [pltpu.make_async_copy(hidden_in, hidden, lsem.at[5]), pltpu.make_async_copy(lens_in, lens, lsem.at[6])]
    for copy in small:
        copy.start()
    for _, _, copy in loads[:in_flight]:
        copy.start()

    barrier = pltpu.get_barrier_semaphore()
    for dy in range(ny):
        for ds in range(ns):
            if dy or ds:
                pl.semaphore_signal(barrier, inc=1, device_id={"ctx": (y + dy) % ny, "seq": (s + ds) % ns},
                                    device_id_type=MESH)

    for copy in small:
        copy.wait()
    wide_k = step * half_h
    si = lax.broadcasted_iota(jnp.int32, (2 * half_b, nb), 0)
    sj = lax.broadcasted_iota(jnp.int32, (2 * half_b, nb), 1)
    own_rows = jnp.where(sj == rb * half_b + si % half_b, 1.0, 0.0).astype(jnp.bfloat16)
    hid2 = jnp.dot(own_rows, hidden[...], preferred_element_type=jnp.float32).astype(jnp.bfloat16)
    stack = jnp.concatenate([hid2[:, step * k:step * k + step] for k in range(n_step)], axis=0)
    for n in range(half_h):
        ri = lax.broadcasted_iota(jnp.int32, (step, step), 0)
        rj = lax.broadcasted_iota(jnp.int32, (step, step), 1)
        spread = jnp.where(ri == (rj + n * step) // half_h, 1.0, 0.0).astype(jnp.bfloat16)
        hrep[:, n * step:(n + 1) * step] = jnp.dot(stack, spread, preferred_element_type=jnp.float32).astype(jnp.bfloat16)

    pl.semaphore_wait(barrier, ny * ns - 1)

    mate = {"ctx": y, "seq": s + 1 - 2 * c}
    other = pl.ds((1 - c) * t_own, t_own)
    swap = [
        pltpu.make_async_remote_copy(cache, cacheb.at[:, span, pl.ds(0, latent)], csend.at[0], crecv.at[0], device_id=mate, device_id_type=MESH),
        pltpu.make_async_remote_copy(rope, ropeb.at[:, :, span], csend.at[1], crecv.at[1], device_id=mate, device_id_type=MESH),
    ]
    q_rope = []
    lane_h = lax.broadcasted_iota(jnp.int32, (2 * half_b, wide_k), 1) % half_h
    row_h = lax.broadcasted_iota(jnp.int32, (2 * half_b, wide_k), 0) // half_b
    sums = [jnp.zeros((half_h * half_b, nope), jnp.float32) for _ in range(2)]
    for i, (kind, n, copy) in enumerate(loads):
        copy.wait()
        if i + in_flight < len(loads):
            loads[i + in_flight][2].start()
        else:
            k = i + in_flight - len(loads)
            if k < 3:
                local[k].start()
        if i == 5:
            for swap_copy in reversed(swap):
                swap_copy.start()
        if kind == 1:
            half = r_step * rope_dim // 2
            w = wqrb[n * r_step:(n + 1) * r_step].reshape(r_step * rope_dim, d_model)
            for p in range(2):
                q_rope.append(lax.dot_general(w[half * p:half * p + half], hid2, (((1,), (1,)), ((), ())), preferred_element_type=jnp.float32))
        else:
            for k in range(n * group, (n + 1) * group):
                hr = hrep[2 * half_b * k:2 * half_b * (k + 1), :]
                lhs = jnp.concatenate([jnp.where(lane_h == row_h + h, hr, jnp.zeros_like(hr)) for h in range(0, half_h, 2)], axis=0)
                w = wuqb[k * step:(k + 1) * step].reshape(wide_k, nope)
                sums[k % 2] = sums[k % 2] + jnp.dot(lhs, w, preferred_element_type=jnp.float32)
    q_rope = jnp.concatenate(q_rope, axis=0).T
    q_rope = jnp.concatenate([q_rope[0:half_b, rope_dim * h:rope_dim * (h + 1)] for h in range(half_h)], axis=0).astype(jnp.bfloat16)
    q_nope = (sums[0] + sums[1]).astype(jnp.bfloat16)

    n_q = half_b * half_h
    qi = lax.broadcasted_iota(jnp.int32, (n_q, n_q), 0)
    qj = lax.broadcasted_iota(jnp.int32, (n_q, n_q), 1)
    pick = jnp.where((qi % half_h == qj // half_b) & (qi // half_h == qj % half_b), 1.0, 0.0).astype(jnp.bfloat16)
    q_nope = jnp.dot(pick, q_nope, preferred_element_type=jnp.float32).astype(jnp.bfloat16)
    q_rope = jnp.dot(pick, q_rope, preferred_element_type=jnp.float32)
    head_of = lax.broadcasted_iota(jnp.int32, (n_q, nope), 0) % half_h
    big = jnp.concatenate([jnp.where(head_of == h, q_nope, jnp.zeros_like(q_nope)) for h in range(half_h)], axis=1)
    local[0].wait()
    q_lat = jnp.dot(big, wukb[...].reshape(half_h * nope, latent), preferred_element_type=jnp.float32).astype(jnp.bfloat16)
    for j in range(half_b // 2):
        for n in range(latent // LANES):
            qbuf[rb, j, hb, x, block(n, PACK), :] = q_lat[block(j, PACK), block(n, LANES)]
        sides = [q_rope[block(2 * j + i, SUB)] for i in range(2)]
        qbuf[rb, j, hb, x, 64:72, :] = jnp.concatenate(sides, axis=1).astype(jnp.bfloat16)


    def send(src, dst, ssem, rsem, to):
        copy = pltpu.make_async_remote_copy(src, dst, ssem, rsem, device_id=to, device_id_type=MESH)
        copy.start()

    def recv(dst, rsem):
        pltpu.make_async_remote_copy(dst, dst, rsem, rsem, device_id=mate, device_id_type=MESH).wait_recv()

    def sent(src, ssem):
        pltpu.make_async_remote_copy(src, src, ssem, ssem, device_id=mate, device_id_type=MESH).wait_send()

    def rbhb(d):
        yy = (y + d + ny) % ny
        return yy // 2, yy % 2

    def xx(d):
        return (x + d + nx) % nx

    def cell(j, d1, d2):
        d_y, d_x = (d2, d1) if j < 2 else (d1, d2)
        r_, h_ = rbhb(-d_y)
        return qbuf.at[r_, j, h_, xx(-d_x)]

    def hop(j, stage, ref, along_x):
        for d in OTHERS:
            send(ref, ref, gsend.at[1 if stage else 0], grecv.at[j, 0 if stage else d], at_x(d) if along_x else at_y(d))

    for a in range(2):
        for j in (a, a + 2):
            hop(j, 0, cell(j, 0, 0), j < 2)
        for j in (a, a + 2):
            hop(j, 1, cell(j, 0, 0), j >= 2)
    for a in range(2):
        for e in reversed(OTHERS):
            for j in (a, a + 2):
                recv(cell(j, e, 0), grecv.at[j, e])
                hop(j, 1 + e, cell(j, e, 0), j >= 2)

    def gather_finish(j):
        recv(qbuf.at[0, 0:3, 0], grecv.at[j, 0])

    for copy in local[3:]:
        copy.start()
    for copy in local[1:3]:
        copy.wait()
    recv(cacheb.at[:, other, pl.ds(0, latent)], crecv.at[0])
    recv(ropeb.at[:, :, other], crecv.at[1])
    for b in range(nb):
        blank = jnp.zeros((LANES - rope_dim, n_pos), jnp.bfloat16)
        keys = jnp.concatenate([blank, ropeb[b]] if b % 2 else [ropeb[b], blank], axis=0)
        cacheb[b, :, latent:] = keys.T
    gather_finish(0)
    gather_finish(2)

    base = (y * ns + 2 * x) * t_own
    n_head = qbuf.shape[2] * qbuf.shape[3] * 8
    lane = lax.broadcasted_iota(jnp.int32, (SUB, LANES), 1)
    n_slab = latent // LANES

    def stats(groups):
        tile = jnp.zeros((SUB, LANES), jnp.float32)
        for i, (m_, l_) in enumerate(groups):
            tile = jnp.where((lane >= 32 * i) & (lane < 32 * i + 16), m_, tile)
            tile = jnp.where((lane >= 32 * i + 16) & (lane < 32 * i + 32), l_, tile)
        return tile

    def attend(*pairs):
        first = lax.broadcasted_iota(jnp.int32, (n_pos, 2 * n_head), 1) % PACK < SUB
        first_row = lax.broadcasted_iota(jnp.int32, (1, 2 * n_head), 1) % PACK < SUB
        pos = lax.broadcasted_iota(jnp.int32, (n_pos, 2 * n_head), 0)
        b0s = [4 * r + 2 * (1 - cls) for cls, r in pairs]
        scores = []
        for (cls, r), b0 in zip(pairs, b0s):
            r_, j_ = r // 2, 1 - cls + 2 * (r % 2)
            slabs = [qbuf[r_, j_, :, :, block(n, PACK), :].reshape(2 * n_head, LANES) for n in range(n_slab)]
            side = qbuf[r_, j_, :, :, 64:72, :]
            side = jnp.concatenate([side, side], axis=2).reshape(2 * n_head, LANES)
            q2 = jnp.concatenate(slabs + [side], axis=1)
            scores.append([lax.dot_general(cacheb[b0 + i], q2, (((1,), (1,)), ((), ())), preferred_element_type=jnp.float32) for i in range(2)])
        res = []
        for sc, b0 in zip(scores, b0s):
            limit = jnp.where(first_row, lens[b0], lens[b0 + 1]) - base
            sc = jnp.where(first, sc[0], sc[1]) * scale
            sc = jnp.where(pos < limit, sc, NEG_FILL)
            m = jnp.maximum(jnp.max(sc, axis=0, keepdims=True), MAX_FLOOR)
            w = jnp.exp(sc - m)
            l = jnp.sum(w, axis=0, keepdims=True)
            res.append((m, l, w.astype(jnp.bfloat16).T))
        new = []
        for (m, l, w), b0 in zip(res, b0s):
            acc = [jnp.dot(w, cacheb[b0 + i, :, 0:latent], preferred_element_type=jnp.float32) for i in range(2)]
            new.append((acc, jnp.concatenate([m, l, jnp.zeros((6, 2 * n_head), jnp.float32)], axis=0).T))
        for (cls, r), (acc, ml_cols) in zip(pairs, new):
            for x_ in range(nx):
                ml = []
                for g in range(4):
                    k = ((g % 2) * nx + x_) * 16 + 8 * (g // 2)
                    ml.append((ml_cols[k:k + SUB, 0:1], ml_cols[k:k + SUB, 1:2]))
                    for n in range(n_slab):
                        part[cls, r, x_, block(4 * n + g, SUB), :] = acc[g // 2][k:k + SUB, block(n, LANES)]
                part[cls, r, x_, block(4 * n_slab, SUB), :] = stats(ml)

    def merge(items):
        new = []
        row = 32 * n_slab
        for own, boxes in items:
            refs = [own] + boxes
            tiles = [ref[row:row + 8, :] for ref in refs]
            ml = []
            for g in range(4):
                ms = [jnp.broadcast_to(t[:, UNIT * g:UNIT * g + 1], (SUB, LANES)) for t in tiles]
                ls = [jnp.broadcast_to(t[:, UNIT * g + PACK:UNIT * g + PACK + 1], (SUB, LANES)) for t in tiles]
                m = ms[0]
                for other_m in ms[1:]:
                    m = jnp.maximum(m, other_m)
                es = [jnp.exp(m_ - m) for m_ in ms]
                l = ls[0] * es[0]
                for l_, e_ in zip(ls[1:], es[1:]):
                    l = l + l_ * e_
                ml.append((m, l))
                for n in range(n_slab):
                    k = 32 * n + 8 * g
                    total = refs[0][k:k + 8, :] * es[0]
                    for ref, e_ in zip(refs[1:], es[1:]):
                        total = total + ref[k:k + 8, :] * e_
                    new.append((own, k, total))
            new.append((own, row, stats(ml)))
        for own, k, value in new:
            own[k:k + 8, :] = value

    def rs_send(cls, r, x_, i, sem, to):
        send(part.at[cls, r, x_], inbox.at[cls, i], rsend.at[0], rrecv.at[cls, sem], to)

    def rs_merge(*items):
        for cls, _, _, i, n, sem in items:
            recv(inbox.at[cls, pl.ds(i, n)], rrecv.at[cls, sem])
        merge([(part.at[cls, r, x_], [inbox.at[cls, i + k] for k in range(n)]) for cls, r, x_, i, n, _ in items])

    def yy(d):
        return (y + d + ny) % ny

    def a_sign(r):
        return 1 - 2 * (r % 2)

    def a_slot(r, sg):
        return 4 + 2 * r + (1 - sg) // 2

    def a_first(r):
        sg = a_sign(r)
        rs_send(0, r, xx(2), r, r, at_x(sg))
        rs_send(0, r, xx(-sg), a_slot(r, -sg), 4 + r, at_x(-sg))

    def a_second(r):
        sg = a_sign(r)
        rs_merge((0, r, xx(sg), r, 1, r))
        rs_send(0, r, xx(sg), a_slot(r, sg), 4 + r, at_x(sg))

    def b_send(d, odd):
        for x_ in range(odd, nx, 2):
            rs_send(1, yy(d), x_, a_slot(x_, d), 4 + x_, at_y(d))

    def b_second(d, odd):
        rs_merge(*[(1, yy(d), x_, x_, 1, x_) for x_ in range(odd, nx, 2)])
        for x_ in range(odd, nx, 2):
            rs_send(1, yy(d), x_, a_slot(x_, d), 4 + x_, at_y(d))

    def pair(cls, r, x_, k):
        return (cls, r, x_, 4 + 2 * k, 2, 4 + k)

    attend((1, yy(2)), (1, yy(1)))
    for x_ in range(nx):
        rs_send(1, yy(2), x_, x_, x_, at_y(1 - 2 * (x_ % 2)))
    b_send(1, 1)
    gather_finish(1)
    gather_finish(3)
    attend((0, yy(2)), (1, yy(-1)))
    a_first(yy(2))
    b_send(-1, 0)
    attend((0, yy(1)), (0, yy(-1)))
    a_first(yy(1))
    a_first(yy(-1))
    attend((0, y), (1, y))
    a_first(y)
    b_second(1, 0)
    b_second(-1, 1)
    a_second(yy(2))
    a_second(yy(1))
    a_second(yy(-1))
    a_second(y)
    for d in OTHERS:
        rs_merge(pair(0, yy(d), x, yy(d)), pair(1, y, xx(d), xx(d)))
        rs_send(0, yy(d), x, 11 + d, 8, at_y(d))
        rs_send(1, y, xx(d), 11 + d, 8, at_x(d))
    rs_merge(pair(0, y, x, y), pair(1, y, x, x))
    rs_merge((0, y, x, 12, 3, 8), (1, y, x, 12, 3, 8))

    rows = []
    for cls in (1, 0):
        own = part.at[cls, y, x]
        st = own[block(4 * n_slab, SUB), :]
        for g in range(4):
            inv = jnp.broadcast_to(st[:, UNIT * g + PACK:UNIT * g + PACK + 1], (SUB, LANES))
            rows.append(jnp.concatenate([own[block(4 * n + g, SUB), :] / inv for n in range(n_slab)], axis=1))
    o_l = jnp.concatenate(rows, axis=0).astype(jnp.bfloat16)
    n_own = o_l.shape[0]
    local[3].wait()
    head_o = lax.broadcasted_iota(jnp.int32, (n_own, wuv.shape[2]), 0) % nh
    v = jnp.zeros((n_own, wuv.shape[2]), jnp.float32)
    for h in range(nh):
        v = jnp.where(head_o == h, jnp.dot(o_l, wuvb[h], preferred_element_type=jnp.float32), v)
    v = v.astype(jnp.bfloat16)
    pi = lax.broadcasted_iota(jnp.int32, (16 * nh, n_own), 0)
    pj = lax.broadcasted_iota(jnp.int32, (16 * nh, n_own), 1)
    perm = jnp.where((pj % nh == pi // 16) & (pj // nh == pi % 16), 1.0, 0.0).astype(jnp.bfloat16)
    vp = jnp.dot(perm, v, preferred_element_type=jnp.float32).astype(jnp.bfloat16)
    lhs = jnp.concatenate([vp[block(h, PACK)] for h in range(nh)], axis=1)
    local[4].wait()
    n_rows = n_own // nh
    others = [(d, f) for d in OTHERS + (0,) for f in range(2) if d or f]
    for d, f in others + [(0, 0)]:
        s_ = xx(d) * 2 + (1 - c if f else c)
        piece = jnp.dot(lhs, woutb[:, pl.ds(pl.multiple_of(s_ * cols, LANES), cols)], preferred_element_type=jnp.float32)
        if (d, f) != (0, 0):
            k = 2 * d + f
            k_there = 2 * ((nx - d) % nx) + f
            ybuf[k] = piece[0:n_rows]
            send(ybuf.at[k], yin.at[k_there], tail_sem.at[0], tail_sem.at[1], {"ctx": y, "seq": s_})
        else:
            total = piece[0:n_rows]
    recv(yin.at[1:ns], tail_sem.at[1])
    for d, f in others:
        total = total + yin[2 * d + f]
    hid = hidden[:, pl.ds(pl.multiple_of(s * cols, LANES), cols)].astype(jnp.float32)
    mine = hid[0:n_rows]
    for y_ in range(1, ny):
        mine = jnp.where(y == y_, hid[n_rows * y_:n_rows * y_ + n_rows], mine)
    obuf[y * ns + s] = (mine + total).astype(jnp.bfloat16)
    me = y * ns + s
    far = [(e, d, f) for e in OTHERS + (0,) for d in OTHERS + (0,) for f in range(2) if e or d or f]
    far.sort(key=lambda t: -(min(t[0], ny - t[0]) + min(t[1], nx - t[1])))
    for e, d, f in far:
        send(obuf.at[me], obuf.at[me], tail_sem.at[2], tail_sem.at[3], {"ctx": yy(e), "seq": xx(d) * 2 + (1 - c if f else c)})
    recv(obuf.at[1:ny * ns], tail_sem.at[3])
    for s_ in range(ns):
        out[:, s_ * cols:(s_ + 1) * cols] = jnp.concatenate(
            [obuf[y_ * ns + s_].astype(jnp.float32) for y_ in range(ny)], axis=0).astype(jnp.bfloat16)
    sent(qbuf.at[0, 0:3, 0], gsend.at[0])
    sent(qbuf.at[:, 0:3], gsend.at[1])
    sent(inbox, rsend.at[0])
    sent(ybuf.at[1:ns], tail_sem.at[0])
    sent(obuf.at[1:ny * ns], tail_sem.at[2])
    for copy in swap:
        copy.wait_send()


def solution(mesh):
    ny, ns = mesh.shape['ctx'], mesh.shape['seq']
    row_spec = P('batch', None)
    cache_spec = P('batch', ('ctx', 'seq'), None)
    proj_spec = P(None, 'seq', None)
    head_spec = P('seq', None, None)

    def local_step(hidden, lengths, latent_cache, rope_keys, w_uq, w_qr, w_uk, w_uv, w_out):
        rope_t = jnp.transpose(rope_keys, (0, 2, 1))
        nb, d_model = hidden.shape
        t_own, latent = latent_cache.shape[1:]
        nh = w_uq.shape[1]
        wqr_t = jnp.transpose(w_qr, (1, 2, 0))
        rope_dim = rope_t.shape[1]
        nx = ns // 2
        cols = d_model // ns
        n_rows = nb // ny
        bf, f32 = jnp.bfloat16, jnp.float32
        unit = (latent // LANES) * 32 + 8
        wide = latent + LANES
        dma = pltpu.SemaphoreType.DMA
        vmem = pl.BlockSpec(memory_space=pltpu.VMEM)
        anyw = pl.BlockSpec(memory_space=pl.ANY)
        import functools
        out = pl.pallas_call(
            functools.partial(decode_kernel, ny, ns),
            out_shape=pltpu.VMEM(hidden.shape, bf),
            in_specs=[anyw, anyw, anyw, anyw, anyw, anyw, anyw, anyw, anyw],
            out_specs=vmem,
            scratch_shapes=[
                pltpu.SMEM(lengths.shape, jnp.int32),
                pltpu.VMEM(hidden.shape, bf),
                pltpu.VMEM((nb, 2 * t_own, wide), bf),
                pltpu.VMEM((nb, rope_dim, 2 * t_own), bf),
                pltpu.VMEM((2, nb // 4, 2, nx, latent // 8 + 8, LANES), bf),
                pltpu.VMEM((2, ny, nx, unit, LANES), f32),
                pltpu.VMEM((2, 15, unit, LANES), f32),
                pltpu.VMEM((nh // 2,) + w_uk.shape[1:], bf),
                pltpu.VMEM(w_uv.shape, bf),
                pltpu.VMEM((w_out.shape[0] * w_out.shape[1], d_model), bf),
                pltpu.VMEM((d_model, nh // 2, w_uq.shape[2]), bf),
                pltpu.VMEM((nh // 2, rope_dim, d_model), bf),
                pltpu.VMEM((d_model // 256 * 16, 256 * nh // 2), bf),
                pltpu.VMEM((ns, n_rows, cols), f32),
                pltpu.VMEM((ns, n_rows, cols), f32),
                pltpu.VMEM((ny * ns, n_rows, cols), bf),
                dma((7,)), dma((d_model // 256,)), dma((nh // 4,)), dma((2,)), dma((2,)), dma((2,)), dma((4, 4)), dma((1,)), dma((2, 9)),
                dma((4,)),
            ],
            compiler_params=pltpu.CompilerParams(collective_id=0, has_side_effects=True, vmem_limit_bytes=60 * 2 ** 20),
        )(lengths, hidden, w_uq.reshape(d_model, 2, nh // 2, -1), wqr_t, w_uk, latent_cache, rope_t, w_uv, w_out.reshape(-1, d_model))
        return out

    return jax.shard_map(local_step, mesh=mesh,
                         in_specs=(row_spec, P('batch'), cache_spec, cache_spec, proj_spec, proj_spec, head_spec, head_spec, head_spec),
                         out_specs=row_spec, check_vma=False)
```

```python
import jax
import jax.numpy as jnp
from jax import lax
from jax.experimental import pallas as pl
from jax.experimental.pallas import tpu as pltpu
from jax.sharding import PartitionSpec as P

NEG_FILL = -3.0e38
MAX_FLOOR = -1.5e38
LANES = 128
MESH = pl.DeviceIdType.MESH
SUB = 8
UNIT = 32
PACK = 16
OTHERS = (2, 1, 3)


def block(i, n):
    return slice(i * n, (i + 1) * n)


def decode_kernel(ny, ns, lens_in, hidden_in, wuq, wqr, wuk, cache, rope, wuv, wout, out,
                  lens, hidden, cacheb, ropeb, qbuf, part, inbox, wukb, wuvb, woutb, wuqb, wqrb, hrep, ybuf, yin, obuf,
                  lsem, usem, qsem, csend, crecv, gsend, grecv, rsend, rrecv, tail_sem):
    nx = ns // 2
    y, s = lax.axis_index("ctx"), lax.axis_index("seq")
    x, c = s // 2, s % 2
    rb, hb = y // 2, y % 2
    t_own, latent = cache.shape[1], cache.shape[2]
    rope_dim = rope.shape[1]
    nope = wuq.shape[3]
    d_model = hidden.shape[1]
    nh = wuk.shape[0]
    half_h = wuq.shape[2]
    nb = hidden.shape[0]
    half_b = nb // 2
    scale = (nope + rope_dim) ** -0.5
    n_pos = 2 * t_own
    cols = hidden.shape[1] // ns

    def at_y(d):
        return {"ctx": (y + d + ny) % ny, "seq": s}

    def at_x(d):
        return {"ctx": y, "seq": ((x + d + nx) % nx) * 2 + c}

    step = 256
    n_step = d_model // step
    r_step = 2
    group = 4
    uq = [pltpu.make_async_copy(wuq.at[pl.ds(k * step * group, step * group), hb], wuqb.at[pl.ds(k * step * group, step * group)], usem.at[k])
          for k in range(n_step // group)]
    qr = [pltpu.make_async_copy(wqr.at[pl.ds(hb * half_h + k * r_step, r_step)], wqrb.at[pl.ds(k * r_step, r_step)], qsem.at[k])
          for k in range(half_h // r_step)]
    span = pl.ds(c * t_own, t_own)
    local = [
        pltpu.make_async_copy(wuk.at[pl.ds(hb * half_h, half_h)], wukb, lsem.at[0]),
        pltpu.make_async_copy(cache, cacheb.at[:, span, pl.ds(0, latent)], lsem.at[1]),
        pltpu.make_async_copy(rope, ropeb.at[:, :, span], lsem.at[2]),
        pltpu.make_async_copy(wuv, wuvb, lsem.at[3]),
        pltpu.make_async_copy(wout, woutb, lsem.at[4]),
    ]
    loads = []
    for k in range(n_step // group):
        if k < half_h // r_step:
            loads.append((1, k, qr[k]))
        loads.append((0, k, uq[k]))
    in_flight = 5
    small = [pltpu.make_async_copy(hidden_in, hidden, lsem.at[5]), pltpu.make_async_copy(lens_in, lens, lsem.at[6])]
    for copy in small:
        copy.start()
    for _, _, copy in loads[:in_flight]:
        copy.start()

    barrier = pltpu.get_barrier_semaphore()
    for dy in range(ny):
        for ds in range(ns):
            if dy or ds:
                pl.semaphore_signal(barrier, inc=1, device_id={"ctx": (y + dy) % ny, "seq": (s + ds) % ns},
                                    device_id_type=MESH)

    for copy in small:
        copy.wait()
    wide_k = step * half_h
    si = lax.broadcasted_iota(jnp.int32, (2 * half_b, nb), 0)
    sj = lax.broadcasted_iota(jnp.int32, (2 * half_b, nb), 1)
    own_rows = jnp.where(sj == rb * half_b + si % half_b, 1.0, 0.0).astype(jnp.bfloat16)
    hid2 = jnp.dot(own_rows, hidden[...], preferred_element_type=jnp.float32).astype(jnp.bfloat16)
    stack = jnp.concatenate([hid2[:, step * k:step * k + step] for k in range(n_step)], axis=0)
    for n in range(half_h):
        ri = lax.broadcasted_iota(jnp.int32, (step, step), 0)
        rj = lax.broadcasted_iota(jnp.int32, (step, step), 1)
        spread = jnp.where(ri == (rj + n * step) // half_h, 1.0, 0.0).astype(jnp.bfloat16)
        hrep[:, n * step:(n + 1) * step] = jnp.dot(stack, spread, preferred_element_type=jnp.float32).astype(jnp.bfloat16)

    pl.semaphore_wait(barrier, ny * ns - 1)

    mate = {"ctx": y, "seq": s + 1 - 2 * c}
    other = pl.ds((1 - c) * t_own, t_own)
    swap = [
        pltpu.make_async_remote_copy(cache, cacheb.at[:, span, pl.ds(0, latent)], csend.at[0], crecv.at[0], device_id=mate, device_id_type=MESH),
        pltpu.make_async_remote_copy(rope, ropeb.at[:, :, span], csend.at[1], crecv.at[1], device_id=mate, device_id_type=MESH),
    ]
    q_rope = []
    lane_h = lax.broadcasted_iota(jnp.int32, (2 * half_b, wide_k), 1) % half_h
    row_h = lax.broadcasted_iota(jnp.int32, (2 * half_b, wide_k), 0) // half_b
    sums = [jnp.zeros((half_h * half_b, nope), jnp.float32) for _ in range(2)]
    for i, (kind, n, copy) in enumerate(loads):
        copy.wait()
        if i + in_flight < len(loads):
            loads[i + in_flight][2].start()
        else:
            k = i + in_flight - len(loads)
            if k < 3:
                local[k].start()
        if i == 5:
            for swap_copy in reversed(swap):
                swap_copy.start()
        if kind == 1:
            half = r_step * rope_dim // 2
            w = wqrb[n * r_step:(n + 1) * r_step].reshape(r_step * rope_dim, d_model)
            for p in range(2):
                q_rope.append(lax.dot_general(w[half * p:half * p + half], hid2, (((1,), (1,)), ((), ())), preferred_element_type=jnp.float32))
        else:
            for k in range(n * group, (n + 1) * group):
                hr = hrep[2 * half_b * k:2 * half_b * (k + 1), :]
                lhs = jnp.concatenate([jnp.where(lane_h == row_h + h, hr, jnp.zeros_like(hr)) for h in range(0, half_h, 2)], axis=0)
                w = wuqb[k * step:(k + 1) * step].reshape(wide_k, nope)
                sums[k % 2] = sums[k % 2] + jnp.dot(lhs, w, preferred_element_type=jnp.float32)
    q_rope = jnp.concatenate(q_rope, axis=0).T
    q_rope = jnp.concatenate([q_rope[0:half_b, rope_dim * h:rope_dim * (h + 1)] for h in range(half_h)], axis=0).astype(jnp.bfloat16)
    q_nope = (sums[0] + sums[1]).astype(jnp.bfloat16)

    n_q = half_b * half_h
    qi = lax.broadcasted_iota(jnp.int32, (n_q, n_q), 0)
    qj = lax.broadcasted_iota(jnp.int32, (n_q, n_q), 1)
    pick = jnp.where((qi % half_h == qj // half_b) & (qi // half_h == qj % half_b), 1.0, 0.0).astype(jnp.bfloat16)
    q_nope = jnp.dot(pick, q_nope, preferred_element_type=jnp.float32).astype(jnp.bfloat16)
    q_rope = jnp.dot(pick, q_rope, preferred_element_type=jnp.float32)
    head_of = lax.broadcasted_iota(jnp.int32, (n_q, nope), 0) % half_h
    big = jnp.concatenate([jnp.where(head_of == h, q_nope, jnp.zeros_like(q_nope)) for h in range(half_h)], axis=1)
    local[0].wait()
    q_lat = jnp.dot(big, wukb[...].reshape(half_h * nope, latent), preferred_element_type=jnp.float32).astype(jnp.bfloat16)
    for j in range(half_b // 2):
        for n in range(latent // LANES):
            qbuf[rb, j, hb, x, block(n, PACK), :] = q_lat[block(j, PACK), block(n, LANES)]
        sides = [q_rope[block(2 * j + i, SUB)] for i in range(2)]
        qbuf[rb, j, hb, x, 64:72, :] = jnp.concatenate(sides, axis=1).astype(jnp.bfloat16)


    def send(src, dst, ssem, rsem, to):
        copy = pltpu.make_async_remote_copy(src, dst, ssem, rsem, device_id=to, device_id_type=MESH)
        copy.start()

    def recv(dst, rsem):
        pltpu.make_async_remote_copy(dst, dst, rsem, rsem, device_id=mate, device_id_type=MESH).wait_recv()

    def sent(src, ssem):
        pltpu.make_async_remote_copy(src, src, ssem, ssem, device_id=mate, device_id_type=MESH).wait_send()

    def rbhb(d):
        yy = (y + d + ny) % ny
        return yy // 2, yy % 2

    def xx(d):
        return (x + d + nx) % nx

    def cell(j, d1, d2):
        d_y, d_x = (d2, d1) if j < 2 else (d1, d2)
        r_, h_ = rbhb(-d_y)
        return qbuf.at[r_, j, h_, xx(-d_x)]

    def hop(j, stage, ref, along_x):
        for d in OTHERS:
            send(ref, ref, gsend.at[1 if stage else 0], grecv.at[j, 0 if stage else d], at_x(d) if along_x else at_y(d))

    for a in range(2):
        for j in (a, a + 2):
            hop(j, 0, cell(j, 0, 0), j < 2)
        for j in (a, a + 2):
            hop(j, 1, cell(j, 0, 0), j >= 2)
    for a in range(2):
        for e in (1, 3, 2):
            for j in (a, a + 2):
                recv(cell(j, e, 0), grecv.at[j, e])
                hop(j, 1 + e, cell(j, e, 0), j >= 2)

    def gather_finish(j):
        recv(qbuf.at[0, 0:3, 0], grecv.at[j, 0])

    for copy in local[3:]:
        copy.start()
    for copy in local[1:3]:
        copy.wait()
    recv(cacheb.at[:, other, pl.ds(0, latent)], crecv.at[0])
    recv(ropeb.at[:, :, other], crecv.at[1])
    for b in range(nb):
        blank = jnp.zeros((LANES - rope_dim, n_pos), jnp.bfloat16)
        keys = jnp.concatenate([blank, ropeb[b]] if b % 2 else [ropeb[b], blank], axis=0)
        cacheb[b, :, latent:] = keys.T
    gather_finish(0)
    gather_finish(2)

    base = (y * ns + 2 * x) * t_own
    n_head = qbuf.shape[2] * qbuf.shape[3] * 8
    lane = lax.broadcasted_iota(jnp.int32, (SUB, LANES), 1)
    n_slab = latent // LANES

    def stats(groups):
        tile = jnp.zeros((SUB, LANES), jnp.float32)
        for i, (m_, l_) in enumerate(groups):
            tile = jnp.where((lane >= 32 * i) & (lane < 32 * i + 16), m_, tile)
            tile = jnp.where((lane >= 32 * i + 16) & (lane < 32 * i + 32), l_, tile)
        return tile

    def attend(*pairs):
        first = lax.broadcasted_iota(jnp.int32, (n_pos, 2 * n_head), 1) % PACK < SUB
        first_row = lax.broadcasted_iota(jnp.int32, (1, 2 * n_head), 1) % PACK < SUB
        pos = lax.broadcasted_iota(jnp.int32, (n_pos, 2 * n_head), 0)
        b0s = [4 * r + 2 * (1 - cls) for cls, r in pairs]
        scores = []
        for (cls, r), b0 in zip(pairs, b0s):
            r_, j_ = r // 2, 1 - cls + 2 * (r % 2)
            slabs = [qbuf[r_, j_, :, :, block(n, PACK), :].reshape(2 * n_head, LANES) for n in range(n_slab)]
            side = qbuf[r_, j_, :, :, 64:72, :]
            side = jnp.concatenate([side, side], axis=2).reshape(2 * n_head, LANES)
            q2 = jnp.concatenate(slabs + [side], axis=1)
            scores.append([lax.dot_general(cacheb[b0 + i], q2, (((1,), (1,)), ((), ())), preferred_element_type=jnp.float32) for i in range(2)])
        res = []
        for sc, b0 in zip(scores, b0s):
            limit = jnp.where(first_row, lens[b0], lens[b0 + 1]) - base
            sc = jnp.where(first, sc[0], sc[1]) * scale
            sc = jnp.where(pos < limit, sc, NEG_FILL)
            m = jnp.maximum(jnp.max(sc, axis=0, keepdims=True), MAX_FLOOR)
            w = jnp.exp(sc - m)
            l = jnp.sum(w, axis=0, keepdims=True)
            res.append((m, l, w.astype(jnp.bfloat16).T))
        new = []
        for (m, l, w), b0 in zip(res, b0s):
            acc = [jnp.dot(w, cacheb[b0 + i, :, 0:latent], preferred_element_type=jnp.float32) for i in range(2)]
            new.append((acc, jnp.concatenate([m, l, jnp.zeros((6, 2 * n_head), jnp.float32)], axis=0).T))
        for (cls, r), (acc, ml_cols) in zip(pairs, new):
            for x_ in range(nx):
                ml = []
                for g in range(4):
                    k = ((g % 2) * nx + x_) * 16 + 8 * (g // 2)
                    ml.append((ml_cols[k:k + SUB, 0:1], ml_cols[k:k + SUB, 1:2]))
                    for n in range(n_slab):
                        part[cls, r, x_, block(4 * n + g, SUB), :] = acc[g // 2][k:k + SUB, block(n, LANES)]
                part[cls, r, x_, block(4 * n_slab, SUB), :] = stats(ml)

    def merge(items):
        new = []
        row = 32 * n_slab
        for own, boxes in items:
            refs = [own] + boxes
            tiles = [ref[row:row + 8, :] for ref in refs]
            ml = []
            for g in range(4):
                ms = [jnp.broadcast_to(t[:, UNIT * g:UNIT * g + 1], (SUB, LANES)) for t in tiles]
                ls = [jnp.broadcast_to(t[:, UNIT * g + PACK:UNIT * g + PACK + 1], (SUB, LANES)) for t in tiles]
                m = ms[0]
                for other_m in ms[1:]:
                    m = jnp.maximum(m, other_m)
                es = [jnp.exp(m_ - m) for m_ in ms]
                l = ls[0] * es[0]
                for l_, e_ in zip(ls[1:], es[1:]):
                    l = l + l_ * e_
                ml.append((m, l))
                for n in range(n_slab):
                    k = 32 * n + 8 * g
                    total = refs[0][k:k + 8, :] * es[0]
                    for ref, e_ in zip(refs[1:], es[1:]):
                        total = total + ref[k:k + 8, :] * e_
                    new.append((own, k, total))
            new.append((own, row, stats(ml)))
        for own, k, value in new:
            own[k:k + 8, :] = value

    def rs_send(cls, r, x_, i, sem, to):
        send(part.at[cls, r, x_], inbox.at[cls, i], rsend.at[0], rrecv.at[cls, sem], to)

    def rs_merge(*items):
        for cls, _, _, i, n, sem in items:
            recv(inbox.at[cls, pl.ds(i, n)], rrecv.at[cls, sem])
        merge([(part.at[cls, r, x_], [inbox.at[cls, i + k] for k in range(n)]) for cls, r, x_, i, n, _ in items])

    def yy(d):
        return (y + d + ny) % ny

    def a_sign(r):
        return 1 - 2 * (r % 2)

    def a_slot(r, sg):
        return 4 + 2 * r + (1 - sg) // 2

    def a_first(r):
        sg = a_sign(r)
        rs_send(0, r, xx(2), r, r, at_x(sg))
        rs_send(0, r, xx(-sg), a_slot(r, -sg), 4 + r, at_x(-sg))

    def a_second(r):
        sg = a_sign(r)
        rs_merge((0, r, xx(sg), r, 1, r))
        rs_send(0, r, xx(sg), a_slot(r, sg), 4 + r, at_x(sg))

    def b_send(d, odd):
        for x_ in range(odd, nx, 2):
            rs_send(1, yy(d), x_, a_slot(x_, d), 4 + x_, at_y(d))

    def b_second(d, odd):
        rs_merge(*[(1, yy(d), x_, x_, 1, x_) for x_ in range(odd, nx, 2)])
        for x_ in range(odd, nx, 2):
            rs_send(1, yy(d), x_, a_slot(x_, d), 4 + x_, at_y(d))

    def pair(cls, r, x_, k):
        return (cls, r, x_, 4 + 2 * k, 2, 4 + k)

    attend((1, yy(2)), (1, yy(1)))
    for x_ in range(nx):
        rs_send(1, yy(2), x_, x_, x_, at_y(1 - 2 * (x_ % 2)))
    b_send(1, 1)
    gather_finish(1)
    gather_finish(3)
    attend((0, yy(2)), (1, yy(-1)))
    a_first(yy(2))
    b_send(-1, 0)
    attend((0, yy(1)), (0, yy(-1)))
    a_first(yy(1))
    a_first(yy(-1))
    attend((0, y), (1, y))
    a_first(y)
    b_second(1, 0)
    b_second(-1, 1)
    a_second(yy(2))
    a_second(yy(1))
    a_second(yy(-1))
    a_second(y)
    for d in OTHERS:
        rs_merge(pair(0, yy(d), x, yy(d)), pair(1, y, xx(d), xx(d)))
        rs_send(0, yy(d), x, 11 + d, 8, at_y(d))
        rs_send(1, y, xx(d), 11 + d, 8, at_x(d))
    rs_merge(pair(0, y, x, y), pair(1, y, x, x))
    rs_merge((0, y, x, 12, 3, 8), (1, y, x, 12, 3, 8))

    rows = []
    for cls in (1, 0):
        own = part.at[cls, y, x]
        st = own[block(4 * n_slab, SUB), :]
        for g in range(4):
            inv = jnp.broadcast_to(st[:, UNIT * g + PACK:UNIT * g + PACK + 1], (SUB, LANES))
            rows.append(jnp.concatenate([own[block(4 * n + g, SUB), :] / inv for n in range(n_slab)], axis=1))
    o_l = jnp.concatenate(rows, axis=0).astype(jnp.bfloat16)
    n_own = o_l.shape[0]
    local[3].wait()
    head_o = lax.broadcasted_iota(jnp.int32, (n_own, wuv.shape[2]), 0) % nh
    v = jnp.zeros((n_own, wuv.shape[2]), jnp.float32)
    for h in range(nh):
        v = jnp.where(head_o == h, jnp.dot(o_l, wuvb[h], preferred_element_type=jnp.float32), v)
    v = v.astype(jnp.bfloat16)
    pi = lax.broadcasted_iota(jnp.int32, (16 * nh, n_own), 0)
    pj = lax.broadcasted_iota(jnp.int32, (16 * nh, n_own), 1)
    perm = jnp.where((pj % nh == pi // 16) & (pj // nh == pi % 16), 1.0, 0.0).astype(jnp.bfloat16)
    vp = jnp.dot(perm, v, preferred_element_type=jnp.float32).astype(jnp.bfloat16)
    lhs = jnp.concatenate([vp[block(h, PACK)] for h in range(nh)], axis=1)
    local[4].wait()
    n_rows = n_own // nh
    others = [(d, f) for d in OTHERS + (0,) for f in range(2) if d or f]
    for d, f in others + [(0, 0)]:
        s_ = xx(d) * 2 + (1 - c if f else c)
        piece = jnp.dot(lhs, woutb[:, pl.ds(pl.multiple_of(s_ * cols, LANES), cols)], preferred_element_type=jnp.float32)
        if (d, f) != (0, 0):
            k = 2 * d + f
            k_there = 2 * ((nx - d) % nx) + f
            ybuf[k] = piece[0:n_rows]
            send(ybuf.at[k], yin.at[k_there], tail_sem.at[0], tail_sem.at[1], {"ctx": y, "seq": s_})
        else:
            total = piece[0:n_rows]
    recv(yin.at[1:ns], tail_sem.at[1])
    for d, f in others:
        total = total + yin[2 * d + f]
    hid = hidden[:, pl.ds(pl.multiple_of(s * cols, LANES), cols)].astype(jnp.float32)
    mine = hid[0:n_rows]
    for y_ in range(1, ny):
        mine = jnp.where(y == y_, hid[n_rows * y_:n_rows * y_ + n_rows], mine)
    obuf[y * ns + s] = (mine + total).astype(jnp.bfloat16)
    me = y * ns + s
    far = [(e, d, f) for e in OTHERS + (0,) for d in OTHERS + (0,) for f in range(2) if e or d or f]
    far.sort(key=lambda t: -(min(t[0], ny - t[0]) + min(t[1], nx - t[1])))
    for e, d, f in far:
        send(obuf.at[me], obuf.at[me], tail_sem.at[2], tail_sem.at[3], {"ctx": yy(e), "seq": xx(d) * 2 + (1 - c if f else c)})
    recv(obuf.at[1:ny * ns], tail_sem.at[3])
    for s_ in range(ns):
        out[:, s_ * cols:(s_ + 1) * cols] = jnp.concatenate(
            [obuf[y_ * ns + s_].astype(jnp.float32) for y_ in range(ny)], axis=0).astype(jnp.bfloat16)
    sent(qbuf.at[0, 0:3, 0], gsend.at[0])
    sent(qbuf.at[:, 0:3], gsend.at[1])
    sent(inbox, rsend.at[0])
    sent(ybuf.at[1:ns], tail_sem.at[0])
    sent(obuf.at[1:ny * ns], tail_sem.at[2])
    for copy in swap:
        copy.wait_send()


def solution(mesh):
    ny, ns = mesh.shape['ctx'], mesh.shape['seq']
    row_spec = P('batch', None)
    cache_spec = P('batch', ('ctx', 'seq'), None)
    proj_spec = P(None, 'seq', None)
    head_spec = P('seq', None, None)

    def local_step(hidden, lengths, latent_cache, rope_keys, w_uq, w_qr, w_uk, w_uv, w_out):
        rope_t = jnp.transpose(rope_keys, (0, 2, 1))
        nb, d_model = hidden.shape
        t_own, latent = latent_cache.shape[1:]
        nh = w_uq.shape[1]
        wqr_t = jnp.transpose(w_qr, (1, 2, 0))
        rope_dim = rope_t.shape[1]
        nx = ns // 2
        cols = d_model // ns
        n_rows = nb // ny
        bf, f32 = jnp.bfloat16, jnp.float32
        unit = (latent // LANES) * 32 + 8
        wide = latent + LANES
        dma = pltpu.SemaphoreType.DMA
        vmem = pl.BlockSpec(memory_space=pltpu.VMEM)
        anyw = pl.BlockSpec(memory_space=pl.ANY)
        import functools
        out = pl.pallas_call(
            functools.partial(decode_kernel, ny, ns),
            out_shape=pltpu.VMEM(hidden.shape, bf),
            in_specs=[anyw, anyw, anyw, anyw, anyw, anyw, anyw, anyw, anyw],
            out_specs=vmem,
            scratch_shapes=[
                pltpu.SMEM(lengths.shape, jnp.int32),
                pltpu.VMEM(hidden.shape, bf),
                pltpu.VMEM((nb, 2 * t_own, wide), bf),
                pltpu.VMEM((nb, rope_dim, 2 * t_own), bf),
                pltpu.VMEM((2, nb // 4, 2, nx, latent // 8 + 8, LANES), bf),
                pltpu.VMEM((2, ny, nx, unit, LANES), f32),
                pltpu.VMEM((2, 15, unit, LANES), f32),
                pltpu.VMEM((nh // 2,) + w_uk.shape[1:], bf),
                pltpu.VMEM(w_uv.shape, bf),
                pltpu.VMEM((w_out.shape[0] * w_out.shape[1], d_model), bf),
                pltpu.VMEM((d_model, nh // 2, w_uq.shape[2]), bf),
                pltpu.VMEM((nh // 2, rope_dim, d_model), bf),
                pltpu.VMEM((d_model // 256 * 16, 256 * nh // 2), bf),
                pltpu.VMEM((ns, n_rows, cols), f32),
                pltpu.VMEM((ns, n_rows, cols), f32),
                pltpu.VMEM((ny * ns, n_rows, cols), bf),
                dma((7,)), dma((d_model // 256,)), dma((nh // 4,)), dma((2,)), dma((2,)), dma((2,)), dma((4, 4)), dma((1,)), dma((2, 9)),
                dma((4,)),
            ],
            compiler_params=pltpu.CompilerParams(collective_id=0, has_side_effects=True, vmem_limit_bytes=60 * 2 ** 20),
        )(lengths, hidden, w_uq.reshape(d_model, 2, nh // 2, -1), wqr_t, w_uk, latent_cache, rope_t, w_uv, w_out.reshape(-1, d_model))
        return out

    return jax.shard_map(local_step, mesh=mesh,
                         in_specs=(row_spec, P('batch'), cache_spec, cache_spec, proj_spec, proj_spec, head_spec, head_spec, head_spec),
                         out_specs=row_spec, check_vma=False)
```
